1024 devices in a mesh: sfc: 64 (over z, core), lev: 16 (over x, y).
Axes of the slice: x: 4, y: 4, z: 32, core: 2. Of those that a mesh axis runs over, the one named last changes fastest.
Arguments:
- tracer_old: float32 [16, 10, 16, 24576], P('lev', None, None, 'sfc'), may hold values from 0.1 to 2
- air_old: float32 [16, 16, 24576], P('lev', None, 'sfc'), may hold values from 0.3 to 20, as said below
- air_new: float32 [16, 16, 24576], P('lev', None, 'sfc'), may hold values from 0.4 to 20, as said below
- dep_coord: float32 [2, 16, 16, 24576], P(None, 'lev', None, 'sfc'), may hold values from -1 to 1
- dep_slot: int32 [16, 16, 24576], P('lev', None, 'sfc'), may hold values from 0 to 639
- fetch_list: int32 [64, 2, 128], P('sfc'), may hold values from 0 to 383, as said below
Outputs:
- tracer_new: float32 [16, 10, 16, 24576], P('lev', None, None, 'sfc')
The draws below stay inside these ranges and needn't reach their ends.
Inputs may be any that keep to these rules, and one draw needn't show every extreme that they name: `fetch_list`: side 0 holds distinct indices in [128, 384); side 1 holds distinct indices in [0, 256). `air_old`: positive. `air_new`: positive.
All inputs are finite; a program needn't handle non-finite values.
Results may differ from the reference program's by a relative error of at most 0.0003.
Values sent between devices are 32-bit elements; how exact they have to be, the bound alone decides.
No kernel may reach another device: no remote copies, remote signals or barrier semaphores. Data moves between devices by JAX's collectives and lax.ppermute only.
A program may use at most 32 MiB of HBM per device.

```python
import math
import jax
import jax.numpy as jnp
from jax import lax

NP2 = 16
TRACERS = 10
E_DEV = 384
CAP = 128
BAND = 256
SEGS = 64
ELEMS = 24576
LEVELS = 16


def air_ramp():
    levels = jnp.arange(LEVELS, dtype=jnp.float32)
    elems = jnp.arange(ELEMS, dtype=jnp.float32)
    down = 1.0 + 2.0 * levels / max(LEVELS - 1, 1)
    along = 1.0 + 2.0 * elems / ELEMS
    return down[:, None, None] * along[None, None, :]


def draw_air_old(key, part):
    shape = (LEVELS, NP2, ELEMS)
    common = jax.random.uniform(jax.random.fold_in(key, 5), (), jnp.float32, 0.75, 1.25)
    base = jax.random.uniform(key, shape, jnp.float32, 0.8, 1.2)
    return common * base * air_ramp()


def draw_air_new(key, part):
    shape = (LEVELS, NP2, ELEMS)
    inner = jax.random.fold_in(key, 7)
    base = jax.random.uniform(inner, shape, jnp.float32, 0.72, 1.08)
    return base * air_ramp()


def draw_fetch_list(key, part):
    keys = jax.random.split(jax.random.fold_in(key, 11), SEGS * 2)
    orders = jax.vmap(lambda k: jax.random.permutation(k, BAND))(keys)
    picked = orders[:, :CAP].reshape(SEGS, 2, CAP).astype(jnp.int32)
    offset = jnp.array([E_DEV - BAND, 0], dtype=jnp.int32)
    return picked + offset[None, :, None]


def with_ends(values, key, smallest, high):
    longest = values.shape.index(max(values.shape))
    spots = []
    for shift in (0, 1):
        where = [jax.random.randint(jax.random.fold_in(key, axis), (), 0, length) for axis, length in enumerate(values.shape)]
        where[longest] = (where[longest] + shift) % values.shape[longest]
        spots.append(tuple(where))
    return values.at[spots[0]].set(smallest).at[spots[1]].set(high)


def level_of(own_key, dims, shards, smallest, largest):
    factor_of, own = 1.0, jax.random.fold_in(own_key, 6)
    for axis_at, blocks in shards:
        draws = jnp.exp(jax.random.uniform(jax.random.fold_in(own, axis_at), (blocks,), jnp.float32, smallest / len(shards), largest / len(shards)))
        factor_of = factor_of * jnp.repeat(draws, dims[axis_at] // blocks).reshape([-1 if axis == axis_at else 1 for axis in range(len(dims))])
    return factor_of


def setup_inputs(seed: int = 0) -> dict:
    splits = jax.random.split(jax.random.key(seed), 7)
    tracer_old = jnp.clip(jnp.exp(math.log(2.0) - 2.9957323 * jax.random.uniform(splits[0], (LEVELS, TRACERS, NP2, ELEMS), jnp.float32) ** level_of(splits[0], (LEVELS, TRACERS, NP2, ELEMS), ((0, 16), (3, 64)), -0.2, 0.2)), 0.1, 2.0)
    air_old = draw_air_old(jax.random.fold_in(splits[6], 71), 0)
    air_new = draw_air_new(jax.random.fold_in(splits[6], 71), 0)
    dep_coord = jnp.clip(jax.random.uniform(splits[3], (2, LEVELS, NP2, ELEMS), jnp.float32, -1.0, 1.0) * level_of(splits[3], (2, LEVELS, NP2, ELEMS), ((1, 16), (3, 64)), -0.4, 0.0), -1.0, 1.0)
    dep_slot = with_ends(jax.random.randint(splits[4], (LEVELS, NP2, ELEMS), 0, E_DEV + 2 * CAP), jax.random.fold_in(splits[4], 1), 0, (E_DEV + 2 * CAP) - 1).astype(jnp.int32)
    fetch_list = draw_fetch_list(jax.random.fold_in(splits[6], 71), 0)
    return dict(tracer_old=tracer_old, air_old=air_old, air_new=air_new, dep_coord=dep_coord, dep_slot=dep_slot, fetch_list=fetch_list)


NODES = (-1.0, -0.4472135954999579, 0.4472135954999579, 1.0)


def basis(coord):
    terms = []
    for first in range(4):
        term = jnp.ones_like(coord)
        for other in range(4):
            if other != first:
                term = term * (coord - NODES[other]) / (NODES[first] - NODES[other])
        terms.append(term)
    return jnp.stack(terms)


def weights(coord_a, coord_b):
    along_a = basis(coord_a)
    along_b = basis(coord_b)
    stacked = along_a[:, None] * along_b[None, :]
    return stacked.reshape((16,) + coord_a.shape)


def reference(tracer_old, air_old, air_new, dep_coord, dep_slot, fetch_list):
    segs = fetch_list.shape[0]
    total = tracer_old.shape[3]
    e_dev = total // segs
    seg_ids = jnp.arange(segs, dtype=jnp.int32)
    own = seg_ids[:, None] * e_dev + jnp.arange(e_dev, dtype=jnp.int32)[None, :]
    left = ((seg_ids - 1) % segs)[:, None] * e_dev + fetch_list[:, 0]
    right = ((seg_ids + 1) % segs)[:, None] * e_dev + fetch_list[:, 1]
    table = jnp.concatenate([own, left, right], axis=1).astype(jnp.int32)
    seg_of = (jnp.arange(total, dtype=jnp.int32) // e_dev).astype(jnp.int32)
    source = table[seg_of[None, None, :], dep_slot]

    def level(items):
        field, src, coord_a, coord_b = items

        def point(inner):
            index, along_a, along_b = inner
            blocks = jnp.take(field, index, axis=2)
            wts = weights(along_a, along_b)
            value = jnp.sum(wts[None] * blocks, axis=1)
            return value, jnp.min(blocks, axis=1), jnp.max(blocks, axis=1)

        return lax.map(point, (src, coord_a, coord_b))

    interp, low, high = lax.map(level, (tracer_old, source, dep_coord[0], dep_coord[1]))
    interp = jnp.moveaxis(interp, 1, 2)
    low = jnp.moveaxis(low, 1, 2)
    high = jnp.moveaxis(high, 1, 2)
    clipped = jnp.clip(interp, low, high)
    mass_new = air_new[:, None]
    old_mass = jnp.sum(air_old[:, None] * tracer_old, axis=(0, 2, 3))
    clip_mass = jnp.sum(mass_new * clipped, axis=(0, 2, 3))
    room_up = jnp.sum(mass_new * (high - clipped), axis=(0, 2, 3))
    room_down = jnp.sum(mass_new * (clipped - low), axis=(0, 2, 3))
    shortfall = (old_mass - clip_mass)[None, :, None, None]
    raised = shortfall * (high - clipped) / room_up[None, :, None, None]
    lowered = shortfall * (clipped - low) / room_down[None, :, None, None]
    return clipped + jnp.where(shortfall >= 0, raised, lowered)
```

```python
import functools

import jax
import jax.numpy as jnp
from jax import lax
from jax.experimental import pallas as pl
from jax.experimental.pallas import tpu as pltpu
from jax.sharding import Mesh
from jax.sharding import PartitionSpec as P

BAND = 256
LANES = 128
SFC = ("sfc_0", "sfc_1")
LEV = ("lev_0", "lev_1")
PLANE = ("sfc_1", "lev_0", "lev_1")
LINE = "sfc_0"
NODES = (-1.0, -0.4472135954999579, 0.4472135954999579, 1.0)
UNROLL = 4
GRANT = 12 * 1024 * 1024


def basis(coord):
    terms = []
    for first in range(4):
        term, scale = None, 1.0
        for other in range(4):
            if other != first:
                factor = coord - NODES[other]
                term = factor if term is None else term * factor
                scale *= NODES[first] - NODES[other]
        terms.append(term * (1.0 / scale))
    return terms


def rows(v):
    return pl.ds(v, 8, stride=16) if v < 16 else pl.ds(128 + v - 16, 8, stride=4)


def pick(table, idx):
    return jnp.take_along_axis(table, idx, axis=1, mode="promise_in_bounds")


def group_of_four(x, op):
    y = op(x, pltpu.roll(x, 7, 0))
    return op(y, pltpu.roll(y, 6, 0))


def all_sublanes(x):
    for shift in (4, 2, 1):
        x = x + pltpu.roll(x, shift, 0)
    return x


def interpolate(
    own, air_old, air_new, coord, slot, fetch, left, right,
    clip_out, up_out, down_out, sums_out,
    wide, table, along_a, along_b, stacked, slots, airs,
):
    chunks = own.shape[1] // LANES
    points = slot.shape[0]
    sub = lax.broadcasted_iota(jnp.int32, (8, LANES), 0)
    lane = lax.broadcasted_iota(jnp.int32, (8, LANES), 1)
    for c in range(chunks):
        wide[c] = own[:, c * LANES : (c + 1) * LANES]
    for side, band in enumerate((left, right)):
        for c in range(2):
            wide[chunks + 2 * side + c] = band[:, c * LANES : (c + 1) * LANES]
    old = jnp.zeros((8, LANES), jnp.float32)
    for c in range(chunks):
        air = air_old[:, c * LANES : (c + 1) * LANES]
        for v in range(20):
            x = wide[c, rows(v), :]
            table[c, 8 * v : 8 * v + 8, :] = x
            if v < 16:
                old = old + x * jnp.broadcast_to(air[v : v + 1], (8, LANES))
    tails = []
    for t in (8, 9):
        total = jnp.zeros((8, LANES), jnp.float32)
        for c in range(chunks):
            for h in (0, 8):
                cols = slice(c * LANES, (c + 1) * LANES)
                total = total + wide[c, t * 16 + h : t * 16 + h + 8, :] * air_old[h : h + 8, cols]
        tails.append(all_sublanes(total))
    zero = jnp.zeros((8, LANES), jnp.float32)
    old_tail = jnp.where(sub == 0, tails[0], jnp.where(sub == 4, tails[1], zero))
    for side, shift in enumerate((chunks * LANES - BAND, 0)):
        idx = jnp.broadcast_to(fetch[side : side + 1, :] - shift, (8, LANES))
        near, far = idx & (LANES - 1), idx >= LANES
        for v in range(20):
            first = pick(wide[chunks + 2 * side, rows(v), :], near)
            second = pick(wide[chunks + 2 * side + 1, rows(v), :], near)
            table[chunks + side, 8 * v : 8 * v + 8, :] = jnp.where(far, second, first)
    terms_a = basis(coord[0])
    terms_b = basis(coord[1])
    for c in range(chunks):
        cols = slice(c * LANES, (c + 1) * LANES)
        slots[c] = slot[:, cols]
        airs[c] = air_new[:, cols]
        for i in range(4):
            along_a[i, c] = terms_a[i][:, cols]
            along_b[i, c] = terms_b[i][:, cols]
            stacked[c, pl.ds(i, points, stride=8), :] = terms_a[i][:, cols]
            stacked[c, pl.ds(i + 4, points, stride=8), :] = terms_a[i][:, cols]

    def group(n, e, acc):
        where = jnp.broadcast_to(slots[e, pl.ds(n, 1), :], (8, LANES))
        near, chunk = where & (LANES - 1), where >> 7
        masks = [chunk == c for c in range(1, chunks + 2)]

        def value(v):
            x = pick(table[0, 8 * v : 8 * v + 8, :], near)
            for c, mask in enumerate(masks):
                x = jnp.where(mask, pick(table[c + 1, 8 * v : 8 * v + 8, :], near), x)
            return x

        def row(ref, *at):
            return jnp.broadcast_to(ref[(*at, pl.ds(n, 1), slice(None))], (8, LANES))

        def inner(first):
            total = low = high = None
            for q in range(4):
                x = value(first + q)
                low = x if low is None else jnp.minimum(low, x)
                high = x if high is None else jnp.maximum(high, x)
                term = row(along_b, q, e) * x
                total = term if total is None else total + term
            return total, low, high

        interp, low, high = inner(0)
        interp = interp * row(along_a, 0, e)
        for i in range(1, 4):
            more, least, most = inner(4 * i)
            interp = interp + row(along_a, i, e) * more
            low, high = jnp.minimum(low, least), jnp.maximum(high, most)
        tail, tail_low, tail_high = inner(16)
        tail = tail * stacked[e, pl.ds(pl.multiple_of(8 * n, 8), 8), :]
        tail = group_of_four(tail, jnp.add)
        tail_low = group_of_four(tail_low, jnp.minimum)
        tail_high = group_of_four(tail_high, jnp.maximum)
        air = row(airs, e)
        acc = list(acc)
        for h, (f, lo, hi) in enumerate(((interp, low, high), (tail, tail_low, tail_high))):
            f = jnp.minimum(jnp.maximum(f, lo), hi)
            up, down = hi - f, f - lo
            clip_out[n, e, 8 * h : 8 * h + 8, :] = f
            up_out[n, e, 8 * h : 8 * h + 8, :] = up
            down_out[n, e, 8 * h : 8 * h + 8, :] = down
            acc[3 * h] = acc[3 * h] - air * f
            acc[3 * h + 1] = acc[3 * h + 1] + air * up
            acc[3 * h + 2] = acc[3 * h + 2] + air * down
        return tuple(acc)

    def step(k, acc):
        for u in range(UNROLL):
            for e in range(chunks):
                acc = group(k * UNROLL + u, e, acc)
        return acc

    acc = lax.fori_loop(0, points // UNROLL, step, (old, zero, zero, old_tail, zero, zero))
    row_of = zero
    for k in range(6):
        total = jnp.broadcast_to(jnp.sum(acc[k], axis=1, keepdims=True), (8, LANES))
        keep = lane == 8 * k + sub
        if k >= 3:
            keep = keep & ((sub & 3) == 0)
        row_of = row_of + jnp.where(keep, total, zero)
    row_of = all_sublanes(row_of)
    for k in range(sums_out.shape[0] // 8):
        sums_out[8 * k : 8 * k + 8, :] = row_of


def add_rows(parts):
    total = parts[0:8, :]
    for k in range(1, parts.shape[0] // 8):
        total = total + parts[8 * k : 8 * k + 8, :]
    return all_sublanes(total)


def relay(parts, sums_out):
    total = add_rows(parts)
    for k in range(sums_out.shape[0] // 8):
        sums_out[8 * k : 8 * k + 8, :] = total


def finish(parts, clip, up, down, new_out, wide):
    sub = lax.broadcasted_iota(jnp.int32, (8, LANES), 0)
    lane = lax.broadcasted_iota(jnp.int32, (8, LANES), 1)
    total = add_rows(parts)
    sums = []
    for k in range(6):
        mine = jnp.where(lane == 8 * k + sub, total, jnp.zeros_like(total))
        sums.append(jnp.broadcast_to(jnp.sum(mine, axis=1, keepdims=True), (8, LANES)))
    ratios = []
    for h in range(2):
        short, room_up, room_down = sums[3 * h : 3 * h + 3]
        raised = short >= 0
        zero = jnp.zeros_like(short)
        ratios.append(
            (jnp.where(raised, short / room_up, zero), jnp.where(raised, zero, short / room_down))
        )
    for n in range(clip.shape[0]):
        for e in range(clip.shape[1]):
            for h in range(2):
                at = (n, e, slice(8 * h, 8 * h + 8), slice(None))
                new = clip[at] + ratios[h][0] * up[at] + ratios[h][1] * down[at]
                if h == 0:
                    wide[e, pl.ds(n, 8, stride=16), :] = new
                else:
                    wide[e, 128 + n : 129 + n, :] = new[0:1]
                    wide[e, 144 + n : 145 + n, :] = new[4:5]
    for e in range(clip.shape[1]):
        new_out[:, e * LANES : (e + 1) * LANES] = wide[e]


def in_vmem(kernel, out_shape, count, scratch=()):
    spec = pl.BlockSpec(memory_space=pltpu.VMEM)
    return pl.pallas_call(
        kernel,
        out_shape=out_shape,
        in_specs=[spec] * count,
        out_specs=jax.tree.map(lambda _: spec, out_shape),
        scratch_shapes=scratch,
        compiler_params=pltpu.CompilerParams(vmem_limit_bytes=GRANT),
    )


def on_device(tracer_old, air_old, air_new, dep_coord, dep_slot, fetch_list):
    _, tracers, points, e_dev = tracer_old.shape
    chunks = e_dev // LANES
    real = tracer_old.dtype
    field = tracer_old.reshape(tracers * points, e_dev)
    count = lax.axis_size(SFC)
    forward = [(i, (i + 1) % count) for i in range(count)]
    backward = [(target, source) for source, target in forward]
    left = lax.ppermute(field[:, e_dev - BAND :], SFC, forward)
    right = lax.ppermute(field[:, :BAND], SFC, backward)
    mid = jax.ShapeDtypeStruct((points, chunks, 16, LANES), real)
    plane, line = lax.axis_size(PLANE), lax.axis_size(LINE)
    call = in_vmem(
        interpolate,
        (mid, mid, mid, jax.ShapeDtypeStruct((plane, LANES), real)),
        8,
        [
            pltpu.VMEM((chunks + 4, tracers * points, LANES), real),
            pltpu.VMEM((chunks + 2, 160, LANES), real),
            pltpu.VMEM((4, chunks, points, LANES), real),
            pltpu.VMEM((4, chunks, points, LANES), real),
            pltpu.VMEM((chunks, 8 * points, LANES), real),
            pltpu.VMEM((chunks, points, LANES), jnp.int32),
            pltpu.VMEM((chunks, points, LANES), real),
        ],
    )
    clip, up, down, sums = call(
        field, air_old[0], air_new[0], dep_coord[:, 0], dep_slot[0], fetch_list[0], left, right
    )
    sums = lax.all_to_all(sums, PLANE, 0, 0, tiled=True)
    sums = in_vmem(relay, jax.ShapeDtypeStruct((line, LANES), real), 1)(sums)
    sums = lax.all_to_all(sums, LINE, 0, 0, tiled=True)
    new = in_vmem(
        finish,
        jax.ShapeDtypeStruct((tracers * points, e_dev), real),
        4,
        [pltpu.VMEM((chunks, tracers * points, LANES), real)],
    )(sums, clip, up, down)
    return new.reshape(tracer_old.shape)


def solution(mesh):
    finer = Mesh(mesh.devices.reshape(32, 2, 4, 4), ("sfc_0", "sfc_1", "lev_0", "lev_1"))
    placed = (
        P(LEV, None, None, SFC),
        P(LEV, None, SFC),
        P(LEV, None, SFC),
        P(None, LEV, None, SFC),
        P(LEV, None, SFC),
        P(SFC, None, None),
    )
    return jax.shard_map(
        on_device, mesh=finer, in_specs=placed, out_specs=P(LEV, None, None, SFC), check_vma=False
    )
```

```python
import jax
import jax.numpy as jnp
from jax import lax
from jax.experimental import pallas as pl
from jax.experimental.pallas import tpu as pltpu
from jax.sharding import Mesh
from jax.sharding import PartitionSpec as P

BAND = 256
LANES = 128
SFC = ("sfc_0", "sfc_1")
LEV = ("lev_0", "lev_1")
PLANE = ("sfc_1", "lev_0", "lev_1")
LINE = "sfc_0"
NODES = (-1.0, -0.4472135954999579, 0.4472135954999579, 1.0)
UNROLL = 4
GRANT = 12 * 1024 * 1024
WORK = 10_000_000


def basis(coord):
    terms = []
    for first in range(4):
        term, scale = None, 1.0
        for other in range(4):
            if other != first:
                factor = coord - NODES[other]
                term = factor if term is None else term * factor
                scale *= NODES[first] - NODES[other]
        terms.append(term * (1.0 / scale))
    return terms


def rows(v):
    return pl.ds(v, 8, stride=16) if v < 16 else pl.ds(128 + v - 16, 8, stride=4)


def pick(table, idx):
    return jnp.take_along_axis(table, idx, axis=1, mode="promise_in_bounds")


def group_of_four(x, op):
    y = op(x, pltpu.roll(x, 7, 0))
    return op(y, pltpu.roll(y, 6, 0))


def all_sublanes(x):
    for shift in (4, 2, 1):
        x = x + pltpu.roll(x, shift, 0)
    return x


def old_mass(field, air_old, table, sub):
    zero = jnp.zeros((8, LANES), jnp.float32)
    old = zero
    for c in range(table.shape[0]):
        cols = slice(c * LANES, (c + 1) * LANES)
        for v in range(16):
            air = jnp.broadcast_to(air_old[v : v + 1, cols], (8, LANES))
            old = old + table[c, 8 * v : 8 * v + 8, :] * air
    tails = []
    for t in (8, 9):
        total = zero
        for c in range(table.shape[0]):
            cols = slice(c * LANES, (c + 1) * LANES)
            for h in (0, 8):
                total = total + field[t * 16 + h : t * 16 + h + 8, cols] * air_old[h : h + 8, cols]
        tails.append(all_sublanes(total))
    return old, jnp.where(sub == 0, tails[0], jnp.where(sub == 4, tails[1], zero))


def gather(value, row, stack):
    along_a, along_b = row

    def inner(first):
        total = low = high = None
        for q in range(4):
            x = value(first + q)
            low = x if low is None else jnp.minimum(low, x)
            high = x if high is None else jnp.maximum(high, x)
            term = along_b[q] * x
            total = term if total is None else total + term
        return total, low, high

    interp, low, high = inner(0)
    interp = interp * along_a[0]
    for i in range(1, 4):
        more, least, most = inner(4 * i)
        interp = interp + along_a[i] * more
        low, high = jnp.minimum(low, least), jnp.maximum(high, most)
    tail, tail_low, tail_high = inner(16)
    tail = group_of_four(tail * stack, jnp.add)
    tail_low = group_of_four(tail_low, jnp.minimum)
    tail_high = group_of_four(tail_high, jnp.maximum)
    return (interp, low, high), (tail, tail_low, tail_high)


def broadcast_row(ref, n, *at):
    return jnp.broadcast_to(ref[(*at, pl.ds(n, 1), slice(None))], (8, LANES))


def own_part(
    field, air_old, air_new, coord, slot, fetch,
    picks, interp_out, low_out, high_out, old_out, along_a, along_b, stacked, slots, airs,
    wide, table,
):
    chunks = field.shape[1] // LANES
    points = slot.shape[0]
    sub = lax.broadcasted_iota(jnp.int32, (8, LANES), 0)
    odd = lax.axis_index("sfc_1")
    for side in range(2):
        right = odd if side == 0 else 1 - odd
        start = (chunks * LANES - BAND) * (1 - right)
        mine = jnp.where(right == 1, fetch[1:2, :], fetch[0:1, :]) - start
        picks[side] = jnp.broadcast_to(mine, (8, LANES))
    for c in range(chunks):
        wide[c] = field[:, c * LANES : (c + 1) * LANES]
    for c in range(chunks):
        for v in range(20):
            table[c, 8 * v : 8 * v + 8, :] = wide[c, rows(v), :]
    old_out[0], old_out[1] = old_mass(field, air_old, table, sub)
    terms_a = basis(coord[0])
    terms_b = basis(coord[1])
    for c in range(chunks):
        cols = slice(c * LANES, (c + 1) * LANES)
        slots[c] = slot[:, cols]
        airs[c] = air_new[:, cols]
        for i in range(4):
            along_a[i, c] = terms_a[i][:, cols]
            along_b[i, c] = terms_b[i][:, cols]
            stacked[c, pl.ds(i, points, stride=8), :] = terms_a[i][:, cols]
            stacked[c, pl.ds(i + 4, points, stride=8), :] = terms_a[i][:, cols]

    def step(n, carry):
        for e in range(chunks):
            where = broadcast_row(slots, n, e)
            near, chunk = where & (LANES - 1), where >> 7
            masks = [chunk == c for c in range(1, chunks)]

            def value(v):
                x = pick(table[0, 8 * v : 8 * v + 8, :], near)
                for c, mask in enumerate(masks):
                    x = jnp.where(mask, pick(table[c + 1, 8 * v : 8 * v + 8, :], near), x)
                return x

            row = [[broadcast_row(ref, n, i, e) for i in range(4)] for ref in (along_a, along_b)]
            parts = gather(value, row, stacked[e, pl.ds(pl.multiple_of(8 * n, 8), 8), :])
            for h, part in enumerate(parts):
                for ref, x in zip((interp_out, low_out, high_out), part):
                    ref[n, e, 8 * h : 8 * h + 8, :] = x
        return carry

    lax.fori_loop(0, points, step, 0)


def halo_part(
    across, within, picks, interp, low, high, old, along_a, along_b, stacked, slots, airs,
    clip_out, up_out, down_out, sums_out,
    wide, table,
):
    points, chunks = interp.shape[:2]
    own = chunks * LANES
    sub = lax.broadcasted_iota(jnp.int32, (8, LANES), 0)
    lane = lax.broadcasted_iota(jnp.int32, (8, LANES), 1)
    zero = jnp.zeros((8, LANES), jnp.float32)
    odd = lax.axis_index("sfc_1")
    for k, band in enumerate((across, within)):
        for c in range(2):
            wide[2 * k + c] = band[:, c * LANES : (c + 1) * LANES]
    for side in range(2):
        idx = picks[side]
        near, far = idx & (LANES - 1), idx >= LANES
        for v in range(20):
            first = pick(wide[2 * side, rows(v), :], near)
            second = pick(wide[2 * side + 1, rows(v), :], near)
            table[side, 8 * v : 8 * v + 8, :] = jnp.where(far, second, first)

    def group(n, e, acc):
        where = broadcast_row(slots, n, e)
        near, halo = where & (LANES - 1), where >= own
        at_within = (where >> 7) == chunks + 1 - odd

        def value(v):
            at = slice(8 * v, 8 * v + 8)
            return jnp.where(at_within, pick(table[1, at, :], near), pick(table[0, at, :], near))

        row = [[broadcast_row(ref, n, i, e) for i in range(4)] for ref in (along_a, along_b)]
        parts = gather(value, row, stacked[e, pl.ds(pl.multiple_of(8 * n, 8), 8), :])
        air = broadcast_row(airs, n, e)
        acc = list(acc)
        for h, part in enumerate(parts):
            at = (n, e, slice(8 * h, 8 * h + 8), slice(None))
            f, lo, hi = (
                jnp.where(halo, x, ref[at]) for x, ref in zip(part, (interp, low, high))
            )
            f = jnp.minimum(jnp.maximum(f, lo), hi)
            up, down = hi - f, f - lo
            clip_out[at], up_out[at], down_out[at] = f, up, down
            acc[3 * h] = acc[3 * h] - air * f
            acc[3 * h + 1] = acc[3 * h + 1] + air * up
            acc[3 * h + 2] = acc[3 * h + 2] + air * down
        return tuple(acc)

    def step(k, acc):
        for u in range(UNROLL):
            for e in range(chunks):
                acc = group(k * UNROLL + u, e, acc)
        return acc

    acc = lax.fori_loop(0, points // UNROLL, step, (old[0], zero, zero, old[1], zero, zero))
    row_of = zero
    for k in range(6):
        total = jnp.broadcast_to(jnp.sum(acc[k], axis=1, keepdims=True), (8, LANES))
        keep = lane == 8 * k + sub
        if k >= 3:
            keep = keep & ((sub & 3) == 0)
        row_of = row_of + jnp.where(keep, total, zero)
    row_of = all_sublanes(row_of)
    for k in range(sums_out.shape[0] // 8):
        sums_out[8 * k : 8 * k + 8, :] = row_of


def add_rows(parts):
    total = parts[0:8, :]
    for k in range(1, parts.shape[0] // 8):
        total = total + parts[8 * k : 8 * k + 8, :]
    return all_sublanes(total)


def relay(parts, sums_out):
    total = add_rows(parts)
    for k in range(sums_out.shape[0] // 8):
        sums_out[8 * k : 8 * k + 8, :] = total


def finish(parts, clip, up, down, new_out, wide):
    sub = lax.broadcasted_iota(jnp.int32, (8, LANES), 0)
    lane = lax.broadcasted_iota(jnp.int32, (8, LANES), 1)
    total = add_rows(parts)
    sums = []
    for k in range(6):
        mine = jnp.where(lane == 8 * k + sub, total, jnp.zeros_like(total))
        sums.append(jnp.broadcast_to(jnp.sum(mine, axis=1, keepdims=True), (8, LANES)))
    ratios = []
    for h in range(2):
        short, room_up, room_down = sums[3 * h : 3 * h + 3]
        raised = short >= 0
        zero = jnp.zeros_like(short)
        ratios.append(
            (jnp.where(raised, short / room_up, zero), jnp.where(raised, zero, short / room_down))
        )
    for n in range(clip.shape[0]):
        for e in range(clip.shape[1]):
            for h in range(2):
                at = (n, e, slice(8 * h, 8 * h + 8), slice(None))
                new = clip[at] + ratios[h][0] * up[at] + ratios[h][1] * down[at]
                if h == 0:
                    wide[e, pl.ds(n, 8, stride=16), :] = new
                else:
                    wide[e, 128 + n : 129 + n, :] = new[0:1]
                    wide[e, 144 + n : 145 + n, :] = new[4:5]
    for e in range(clip.shape[1]):
        new_out[:, e * LANES : (e + 1) * LANES] = wide[e]


def in_vmem(kernel, out_shape, count, scratch=(), work=0):
    spec = pl.BlockSpec(memory_space=pltpu.VMEM)
    return pl.pallas_call(
        kernel,
        out_shape=out_shape,
        in_specs=[spec] * count,
        out_specs=jax.tree.map(lambda _: spec, out_shape),
        scratch_shapes=scratch,
        cost_estimate=pl.CostEstimate(flops=work, bytes_accessed=0, transcendentals=0),
        compiler_params=pltpu.CompilerParams(vmem_limit_bytes=GRANT),
    )


def on_device(tracer_old, air_old, air_new, dep_coord, dep_slot, fetch_list):
    _, tracers, points, e_dev = tracer_old.shape
    chunks = e_dev // LANES
    real = tracer_old.dtype
    field = tracer_old.reshape(tracers * points, e_dev)
    count = lax.axis_size(SFC)
    first, last = field[:, :BAND], field[:, e_dev - BAND :]
    even = lax.axis_index("sfc_1") == 0
    across = [(i, (i - 1) % count if i % 2 == 0 else (i + 1) % count) for i in range(count)]
    within = [(i, i + 1 if i % 2 == 0 else i - 1) for i in range(count)]
    got_across = lax.ppermute(jnp.where(even, first, last), SFC, across)
    got_within = lax.ppermute(jnp.where(even, last, first), SFC, within)

    def shape(*dims, dtype=real):
        return jax.ShapeDtypeStruct(dims, dtype)

    mid = shape(points, chunks, 16, LANES)
    plane, line = lax.axis_size(PLANE), lax.axis_size(LINE)
    terms = shape(4, chunks, points, LANES)
    stacked = shape(chunks, 8 * points, LANES)
    slots = shape(chunks, points, LANES, dtype=jnp.int32)
    airs = shape(chunks, points, LANES)
    prepared = in_vmem(
        own_part,
        (shape(2, 8, LANES, dtype=jnp.int32), mid, mid, mid, shape(2, 8, LANES), terms, terms, stacked, slots, airs),
        6,
        [pltpu.VMEM((chunks, tracers * points, LANES), real)] * 2,
        WORK,
    )(field, air_old[0], air_new[0], dep_coord[:, 0], dep_slot[0], fetch_list[0])
    call = in_vmem(
        halo_part,
        (mid, mid, mid, shape(plane, LANES)),
        2 + len(prepared),
        [
            pltpu.VMEM((4, tracers * points, LANES), real),
            pltpu.VMEM((2, 160, LANES), real),
        ],
    )
    clip, up, down, sums = call(got_across, got_within, *prepared)
    sums = lax.all_to_all(sums, PLANE, 0, 0, tiled=True)
    sums = in_vmem(relay, shape(line, LANES), 1)(sums)
    sums = lax.all_to_all(sums, LINE, 0, 0, tiled=True)
    new = in_vmem(
        finish,
        shape(tracers * points, e_dev),
        4,
        [pltpu.VMEM((chunks, tracers * points, LANES), real)],
    )(sums, clip, up, down)
    return new.reshape(tracer_old.shape)


def solution(mesh):
    finer = Mesh(mesh.devices.reshape(32, 2, 4, 4), ("sfc_0", "sfc_1", "lev_0", "lev_1"))
    placed = (
        P(LEV, None, None, SFC),
        P(LEV, None, SFC),
        P(LEV, None, SFC),
        P(None, LEV, None, SFC),
        P(LEV, None, SFC),
        P(SFC, None, None),
    )
    return jax.shard_map(
        on_device, mesh=finer, in_specs=placed, out_specs=P(LEV, None, None, SFC), check_vma=False
    )
```

```python
import jax
import jax.numpy as jnp
from jax import lax
from jax.experimental import pallas as pl
from jax.experimental.pallas import tpu as pltpu
from jax.sharding import Mesh
from jax.sharding import PartitionSpec as P

BAND = 256
LANES = 128
SFC = ("sfc_0", "sfc_1")
LEV = ("lev_0", "lev_1")
PLANE = ("sfc_1", "lev_0", "lev_1")
LINE = "sfc_0"
NODES = (-1.0, -0.4472135954999579, 0.4472135954999579, 1.0)
UNROLL = 2
OWN_UNROLL = 2
STEPS = 32767.0
GRANT = 12 * 1024 * 1024
WORK = 1_000_000_000


def basis(coord):
    terms = []
    for first in range(4):
        term, scale = None, 1.0
        for other in range(4):
            if other != first:
                factor = coord - NODES[other]
                term = factor if term is None else term * factor
                scale *= NODES[first] - NODES[other]
        terms.append(term * (1.0 / scale))
    return terms


def rows(v):
    return pl.ds(v, 8, stride=16) if v < 16 else pl.ds(128 + v - 16, 8, stride=4)


def pick(table, idx):
    return jnp.take_along_axis(table, idx, axis=1, mode="promise_in_bounds")


def group_of_four(x, op):
    y = op(x, pltpu.roll(x, 7, 0))
    return op(y, pltpu.roll(y, 6, 0))


def all_sublanes(x):
    for shift in (4, 2, 1):
        x = x + pltpu.roll(x, shift, 0)
    return x


def old_mass(air_old, wide, sub):
    zero = jnp.zeros((8, LANES), jnp.float32)
    old = zero
    for c in range(wide.shape[0]):
        cols = slice(c * LANES, (c + 1) * LANES)
        for v in range(16):
            air = jnp.broadcast_to(air_old[v : v + 1, cols], (8, LANES))
            old = old + wide[c, rows(v), :] * air
    tails = []
    for t in (8, 9):
        total = zero
        for c in range(wide.shape[0]):
            cols = slice(c * LANES, (c + 1) * LANES)
            for h in (0, 8):
                at = t * 16 + h
                total = total + wide[c, at : at + 8, :] * air_old[h : h + 8, cols]
        tails.append(all_sublanes(total))
    return old, jnp.where(sub == 0, tails[0], jnp.where(sub == 4, tails[1], zero))


def fixed(x):
    return (x * STEPS + 0.5).astype(jnp.int32)


def pair(wide, c, k):
    return fixed(wide[c, rows(2 * k), :]) | (fixed(wide[c, rows(2 * k + 1), :]) << 16)


def halves(x):
    first = (x & 0xFFFF).astype(jnp.float32)
    return first, lax.shift_right_logical(x, 16).astype(jnp.float32)


def gather(pairs, along_a, along_b, stack):
    def inner(first):
        total = low = high = None
        for k in range(2):
            for q, x in enumerate(halves(pairs(first + k))):
                low = x if low is None else jnp.minimum(low, x)
                high = x if high is None else jnp.maximum(high, x)
                term = along_b[2 * k + q] * x
                total = term if total is None else total + term
        return total, low, high

    interp, low, high = inner(0)
    interp = interp * along_a[0]
    for i in range(1, 4):
        more, least, most = inner(2 * i)
        interp = interp + along_a[i] * more
        low, high = jnp.minimum(low, least), jnp.maximum(high, most)
    tail, tail_low, tail_high = inner(8)
    tail = group_of_four(tail * stack, jnp.add)
    tail_low = group_of_four(tail_low, jnp.minimum)
    tail_high = group_of_four(tail_high, jnp.maximum)
    return (interp, low, high), (tail, tail_low, tail_high)


def broadcast_row(ref, n, *at):
    return jnp.broadcast_to(ref[(*at, pl.ds(n, 1), slice(None))], (8, LANES))


def own_part(
    field, air_old, coord, slot, fetch,
    picks, own_out, old_out, along_a, along_b, stacked, slots,
    wide, table,
):
    chunks = slot.shape[1] // LANES
    points = slot.shape[0]
    sub = lax.broadcasted_iota(jnp.int32, (8, LANES), 0)
    for side, start in enumerate((chunks * LANES - BAND, 0)):
        picks[side] = jnp.broadcast_to(fetch[side : side + 1, :] - start, (8, LANES))
    for c in range(chunks):
        wide[c] = field[:, c * LANES : (c + 1) * LANES]
        slots[c] = slot[:, c * LANES : (c + 1) * LANES]
    for c in range(chunks):
        for k in range(10):
            table[c, 8 * k : 8 * k + 8, :] = pair(wide, c, k)

    def step(k, carry):
        for u in range(OWN_UNROLL):
            n = k * OWN_UNROLL + u
            for e in range(chunks):
                where = broadcast_row(slots, n, e)
                near, chunk = where & (LANES - 1), where >> 7
                masks = [chunk == c for c in range(1, chunks)]
                for k2 in range(10):
                    at = slice(8 * k2, 8 * k2 + 8)
                    x = pick(table[0, at, :], near)
                    for c, mask in enumerate(masks):
                        x = jnp.where(mask, pick(table[c + 1, at, :], near), x)
                    own_out[n, e, at, :] = x
        return carry

    lax.fori_loop(0, points // OWN_UNROLL, step, 0)
    old_out[0], old_out[1] = old_mass(air_old, wide, sub)
    terms_a = basis(coord[0])
    terms_b = basis(coord[1])
    for c in range(chunks):
        cols = slice(c * LANES, (c + 1) * LANES)
        for i in range(4):
            along_a[i, c] = terms_a[i][:, cols]
            along_b[i, c] = terms_b[i][:, cols]
            stacked[c, pl.ds(i, points, stride=8), :] = terms_a[i][:, cols]
            stacked[c, pl.ds(i + 4, points, stride=8), :] = terms_a[i][:, cols]


def halo_part(
    left, right, air_new, picks, own, old, along_a, along_b, stacked, slots,
    clip_out, up_out, down_out, sums_out,
    wide, table, airs,
):
    points, chunks = own.shape[:2]
    count = chunks * LANES
    sub = lax.broadcasted_iota(jnp.int32, (8, LANES), 0)
    lane = lax.broadcasted_iota(jnp.int32, (8, LANES), 1)
    zero = jnp.zeros((8, LANES), jnp.float32)
    for c in range(chunks):
        airs[c] = air_new[:, c * LANES : (c + 1) * LANES]
    for side, band in enumerate((left, right)):
        for c in range(2):
            wide[2 * side + c] = band[:, c * LANES : (c + 1) * LANES]
    for side in range(2):
        idx = picks[side]
        near, far = idx & (LANES - 1), idx >= LANES
        for k in range(10):
            first = pick(pair(wide, 2 * side, k), near)
            second = pick(pair(wide, 2 * side + 1, k), near)
            table[side, 8 * k : 8 * k + 8, :] = jnp.where(far, second, first)

    def group(n, e, acc):
        where = broadcast_row(slots, n, e)
        near, at_right, halo = where & (LANES - 1), where >= count + LANES, where >= count

        def pairs(k):
            at = slice(8 * k, 8 * k + 8)
            x = jnp.where(at_right, pick(table[1, at, :], near), pick(table[0, at, :], near))
            return jnp.where(halo, x, own[n, e, at, :])

        row_a, row_b = (
            [broadcast_row(ref, n, i, e) for i in range(4)] for ref in (along_a, along_b)
        )
        parts = gather(pairs, row_a, row_b, stacked[e, pl.ds(pl.multiple_of(8 * n, 8), 8), :])
        air = broadcast_row(airs, n, e)
        acc = list(acc)
        for h, (f, lo, hi) in enumerate(parts):
            at = (n, e, slice(8 * h, 8 * h + 8), slice(None))
            f = jnp.minimum(jnp.maximum(f, lo), hi)
            f, up, down = f * (1.0 / STEPS), (hi - f) * (1.0 / STEPS), (f - lo) * (1.0 / STEPS)
            clip_out[at], up_out[at], down_out[at] = f, up, down
            acc[3 * h] = acc[3 * h] - air * f
            acc[3 * h + 1] = acc[3 * h + 1] + air * up
            acc[3 * h + 2] = acc[3 * h + 2] + air * down
        return tuple(acc)

    def step(k, acc):
        for u in range(UNROLL):
            for e in range(chunks):
                acc = group(k * UNROLL + u, e, acc)
        return acc

    acc = lax.fori_loop(0, points // UNROLL, step, (old[0], zero, zero, old[1], zero, zero))
    row_of = zero
    for k in range(6):
        total = jnp.broadcast_to(jnp.sum(acc[k], axis=1, keepdims=True), (8, LANES))
        keep = lane == 8 * k + sub
        if k >= 3:
            keep = keep & ((sub & 3) == 0)
        row_of = row_of + jnp.where(keep, total, zero)
    row_of = all_sublanes(row_of)
    for k in range(sums_out.shape[0] // 8):
        sums_out[8 * k : 8 * k + 8, :] = row_of


def add_rows(parts):
    total = parts[0:8, :]
    for k in range(1, parts.shape[0] // 8):
        total = total + parts[8 * k : 8 * k + 8, :]
    return all_sublanes(total)


def relay(parts, sums_out):
    total = add_rows(parts)
    for k in range(sums_out.shape[0] // 8):
        sums_out[8 * k : 8 * k + 8, :] = total


def finish(parts, clip, up, down, new_out, wide):
    sub = lax.broadcasted_iota(jnp.int32, (8, LANES), 0)
    lane = lax.broadcasted_iota(jnp.int32, (8, LANES), 1)
    total = add_rows(parts)
    sums = []
    for k in range(6):
        mine = jnp.where(lane == 8 * k + sub, total, jnp.zeros_like(total))
        sums.append(jnp.broadcast_to(jnp.sum(mine, axis=1, keepdims=True), (8, LANES)))
    ratios = []
    for h in range(2):
        short, room_up, room_down = sums[3 * h : 3 * h + 3]
        raised = short >= 0
        zero = jnp.zeros_like(short)
        ratios.append(
            (jnp.where(raised, short / room_up, zero), jnp.where(raised, zero, short / room_down))
        )
    for n in range(clip.shape[0]):
        for e in range(clip.shape[1]):
            for h in range(2):
                at = (n, e, slice(8 * h, 8 * h + 8), slice(None))
                new = clip[at] + ratios[h][0] * up[at] + ratios[h][1] * down[at]
                if h == 0:
                    wide[e, pl.ds(n, 8, stride=16), :] = new
                else:
                    wide[e, 128 + n : 129 + n, :] = new[0:1]
                    wide[e, 144 + n : 145 + n, :] = new[4:5]
    for e in range(clip.shape[1]):
        new_out[:, e * LANES : (e + 1) * LANES] = wide[e]


def in_vmem(kernel, out_shape, count, scratch=(), work=0):
    spec = pl.BlockSpec(memory_space=pltpu.VMEM)
    return pl.pallas_call(
        kernel,
        out_shape=out_shape,
        in_specs=[spec] * count,
        out_specs=jax.tree.map(lambda _: spec, out_shape),
        scratch_shapes=scratch,
        cost_estimate=pl.CostEstimate(flops=work, bytes_accessed=0, transcendentals=0),
        compiler_params=pltpu.CompilerParams(vmem_limit_bytes=GRANT),
    )


def bands(field, last_out, first_out):
    last_out[...] = field[:, field.shape[1] - BAND :]
    first_out[...] = field[:, :BAND]


def on_device(tracer_old, air_old, air_new, dep_coord, dep_slot, fetch_list):
    _, tracers, points, e_dev = tracer_old.shape
    chunks = e_dev // LANES
    real, whole = tracer_old.dtype, jnp.int32
    field = tracer_old.reshape(tracers * points, e_dev)

    def shape(*dims, dtype=real):
        return jax.ShapeDtypeStruct(dims, dtype)

    band = shape(tracers * points, BAND)
    last, first = in_vmem(bands, (band, band), 1, work=WORK)(field)
    count = lax.axis_size(SFC)
    forward = [(i, (i + 1) % count) for i in range(count)]
    backward = [(target, source) for source, target in forward]
    left = lax.ppermute(last, SFC, forward)
    right = lax.ppermute(first, SFC, backward)
    mid = shape(points, chunks, 16, LANES)
    plane, line = lax.axis_size(PLANE), lax.axis_size(LINE)
    terms = shape(4, chunks, points, LANES)
    prepared = in_vmem(
        own_part,
        (
            shape(2, 8, LANES, dtype=whole),
            shape(points, chunks, 80, LANES, dtype=whole),
            shape(2, 8, LANES),
            terms,
            terms,
            shape(chunks, 8 * points, LANES),
            shape(chunks, points, LANES, dtype=whole),
        ),
        5,
        [
            pltpu.VMEM((chunks, tracers * points, LANES), real),
            pltpu.VMEM((chunks, 80, LANES), whole),
        ],
        WORK,
    )(field, air_old[0], dep_coord[:, 0], dep_slot[0], fetch_list[0])
    clip, up, down, sums = in_vmem(
        halo_part,
        (mid, mid, mid, shape(plane, LANES)),
        3 + len(prepared),
        [
            pltpu.VMEM((4, tracers * points, LANES), real),
            pltpu.VMEM((2, 80, LANES), whole),
            pltpu.VMEM((chunks, points, LANES), real),
        ],
    )(left, right, air_new[0], *prepared)
    sums = lax.all_to_all(sums, PLANE, 0, 0, tiled=True)
    sums = in_vmem(relay, shape(line, LANES), 1)(sums)
    sums = lax.all_to_all(sums, LINE, 0, 0, tiled=True)
    new = in_vmem(
        finish,
        shape(tracers * points, e_dev),
        4,
        [pltpu.VMEM((chunks, tracers * points, LANES), real)],
    )(sums, clip, up, down)
    return new.reshape(tracer_old.shape)


def solution(mesh):
    finer = Mesh(mesh.devices.reshape(32, 2, 4, 4), ("sfc_0", "sfc_1", "lev_0", "lev_1"))
    placed = (
        P(LEV, None, None, SFC),
        P(LEV, None, SFC),
        P(LEV, None, SFC),
        P(None, LEV, None, SFC),
        P(LEV, None, SFC),
        P(SFC, None, None),
    )
    return jax.shard_map(
        on_device, mesh=finer, in_specs=placed, out_specs=P(LEV, None, None, SFC), check_vma=False
    )
```

```python
import jax
import jax.numpy as jnp
from jax import lax
from jax.experimental import pallas as pl
from jax.experimental.pallas import tpu as pltpu
from jax.sharding import Mesh
from jax.sharding import PartitionSpec as P

BAND = 256
LANES = 128
SFC = ("far", "near", "core")
LEV = ("lev_0", "lev_1")
CUBE = ("near", "core", "lev_0", "lev_1")
LINE = "far"
ARRIVAL = (0, 1, 3, 6, 7, 5, 4, 2)
NODES = (-1.0, -0.4472135954999579, 0.4472135954999579, 1.0)
UNROLL = 2
OWN_UNROLL = 2
STEPS = 32767.0
GRANT = 12 * 1024 * 1024
WORK = 1_000_000_000


def basis(coord):
    terms = []
    for first in range(4):
        term, scale = None, 1.0
        for other in range(4):
            if other != first:
                factor = coord - NODES[other]
                term = factor if term is None else term * factor
                scale *= NODES[first] - NODES[other]
        terms.append(term * (1.0 / scale))
    return terms


def rows(v):
    return pl.ds(v, 8, stride=16) if v < 16 else pl.ds(128 + v - 16, 8, stride=4)


def pick(table, idx):
    return jnp.take_along_axis(table, idx, axis=1, mode="promise_in_bounds")


def group_of_four(x, op):
    y = op(x, pltpu.roll(x, 7, 0))
    return op(y, pltpu.roll(y, 6, 0))


def all_sublanes(x):
    for shift in (4, 2, 1):
        x = x + pltpu.roll(x, shift, 0)
    return x


def old_mass(air_old, wide, sub):
    zero = jnp.zeros((8, LANES), jnp.float32)
    old = zero
    for c in range(wide.shape[0]):
        cols = slice(c * LANES, (c + 1) * LANES)
        for v in range(16):
            air = jnp.broadcast_to(air_old[v : v + 1, cols], (8, LANES))
            old = old + wide[c, rows(v), :] * air
    tails = []
    for t in (8, 9):
        total = zero
        for c in range(wide.shape[0]):
            cols = slice(c * LANES, (c + 1) * LANES)
            for h in (0, 8):
                at = t * 16 + h
                total = total + wide[c, at : at + 8, :] * air_old[h : h + 8, cols]
        tails.append(all_sublanes(total))
    return old, jnp.where(sub == 0, tails[0], jnp.where(sub == 4, tails[1], zero))


def fixed(x):
    return (x * STEPS + 0.5).astype(jnp.int32)


def pair(wide, c, k):
    return fixed(wide[c, rows(2 * k), :]) | (fixed(wide[c, rows(2 * k + 1), :]) << 16)


def halves(x):
    first = (x & 0xFFFF).astype(jnp.float32)
    return first, lax.shift_right_logical(x, 16).astype(jnp.float32)


def gather(pairs, along_a, along_b, stack):
    def inner(first):
        total = low = high = None
        for k in range(2):
            for q, x in enumerate(halves(pairs(first + k))):
                low = x if low is None else jnp.minimum(low, x)
                high = x if high is None else jnp.maximum(high, x)
                term = along_b[2 * k + q] * x
                total = term if total is None else total + term
        return total, low, high

    interp, low, high = inner(0)
    interp = interp * along_a[0]
    for i in range(1, 4):
        more, least, most = inner(2 * i)
        interp = interp + along_a[i] * more
        low, high = jnp.minimum(low, least), jnp.maximum(high, most)
    tail, tail_low, tail_high = inner(8)
    tail = group_of_four(tail * stack, jnp.add)
    tail_low = group_of_four(tail_low, jnp.minimum)
    tail_high = group_of_four(tail_high, jnp.maximum)
    return (interp, low, high), (tail, tail_low, tail_high)


def broadcast_row(ref, n, *at):
    return jnp.broadcast_to(ref[(*at, pl.ds(n, 1), slice(None))], (8, LANES))


def own_part(
    field, air_old, coord, slot, fetch,
    picks, own_out, old_out, along_a, along_b, stacked, slots,
    wide, table,
):
    chunks = slot.shape[1] // LANES
    points = slot.shape[0]
    sub = lax.broadcasted_iota(jnp.int32, (8, LANES), 0)
    for side, start in enumerate((chunks * LANES - BAND, 0)):
        picks[side] = jnp.broadcast_to(fetch[side : side + 1, :] - start, (8, LANES))
    for c in range(chunks):
        wide[c] = field[:, c * LANES : (c + 1) * LANES]
        slots[c] = slot[:, c * LANES : (c + 1) * LANES]
    for c in range(chunks):
        for k in range(10):
            table[c, 8 * k : 8 * k + 8, :] = pair(wide, c, k)

    def step(k, carry):
        for u in range(OWN_UNROLL):
            n = k * OWN_UNROLL + u
            for e in range(chunks):
                where = broadcast_row(slots, n, e)
                near, chunk = where & (LANES - 1), where >> 7
                masks = [chunk == c for c in range(1, chunks)]
                for k2 in range(10):
                    at = slice(8 * k2, 8 * k2 + 8)
                    x = pick(table[0, at, :], near)
                    for c, mask in enumerate(masks):
                        x = jnp.where(mask, pick(table[c + 1, at, :], near), x)
                    own_out[n, e, at, :] = x
        return carry

    lax.fori_loop(0, points // OWN_UNROLL, step, 0)
    old_out[0], old_out[1] = old_mass(air_old, wide, sub)
    terms_a = basis(coord[0])
    terms_b = basis(coord[1])
    for c in range(chunks):
        cols = slice(c * LANES, (c + 1) * LANES)
        for i in range(4):
            along_a[i, c] = terms_a[i][:, cols]
            along_b[i, c] = terms_b[i][:, cols]
            stacked[c, pl.ds(i, points, stride=8), :] = terms_a[i][:, cols]
            stacked[c, pl.ds(i + 4, points, stride=8), :] = terms_a[i][:, cols]


def halo_part(
    left, right, air_new, picks, own, old, along_a, along_b, stacked, slots,
    clip_out, up_out, down_out, sums_out,
    wide, table, airs,
):
    points, chunks = own.shape[:2]
    count = chunks * LANES
    sub = lax.broadcasted_iota(jnp.int32, (8, LANES), 0)
    lane = lax.broadcasted_iota(jnp.int32, (8, LANES), 1)
    zero = jnp.zeros((8, LANES), jnp.float32)
    for c in range(chunks):
        airs[c] = air_new[:, c * LANES : (c + 1) * LANES]
    for side, band in enumerate((left, right)):
        for c in range(2):
            wide[2 * side + c] = band[:, c * LANES : (c + 1) * LANES]
    for side in range(2):
        idx = picks[side]
        near, far = idx & (LANES - 1), idx >= LANES
        for k in range(10):
            first = pick(pair(wide, 2 * side, k), near)
            second = pick(pair(wide, 2 * side + 1, k), near)
            table[side, 8 * k : 8 * k + 8, :] = jnp.where(far, second, first)

    def group(n, e, acc):
        where = broadcast_row(slots, n, e)
        near, at_right, halo = where & (LANES - 1), where >= count + LANES, where >= count

        def pairs(k):
            at = slice(8 * k, 8 * k + 8)
            x = jnp.where(at_right, pick(table[1, at, :], near), pick(table[0, at, :], near))
            return jnp.where(halo, x, own[n, e, at, :])

        row_a, row_b = (
            [broadcast_row(ref, n, i, e) for i in range(4)] for ref in (along_a, along_b)
        )
        parts = gather(pairs, row_a, row_b, stacked[e, pl.ds(pl.multiple_of(8 * n, 8), 8), :])
        air = broadcast_row(airs, n, e)
        acc = list(acc)
        for h, (f, lo, hi) in enumerate(parts):
            at = (n, e, slice(8 * h, 8 * h + 8), slice(None))
            f = jnp.minimum(jnp.maximum(f, lo), hi)
            f, up, down = f * (1.0 / STEPS), (hi - f) * (1.0 / STEPS), (f - lo) * (1.0 / STEPS)
            clip_out[at], up_out[at], down_out[at] = f, up, down
            acc[3 * h] = acc[3 * h] - air * f
            acc[3 * h + 1] = acc[3 * h + 1] + air * up
            acc[3 * h + 2] = acc[3 * h + 2] + air * down
        return tuple(acc)

    def step(k, acc):
        for u in range(UNROLL):
            for e in range(chunks):
                acc = group(k * UNROLL + u, e, acc)
        return acc

    acc = lax.fori_loop(0, points // UNROLL, step, (old[0], zero, zero, old[1], zero, zero))
    row_of = zero
    for k in range(6):
        total = jnp.broadcast_to(jnp.sum(acc[k], axis=1, keepdims=True), (8, LANES))
        keep = lane == 8 * k + sub
        if k >= 3:
            keep = keep & ((sub & 3) == 0)
        row_of = row_of + jnp.where(keep, total, zero)
    row_of = all_sublanes(row_of)
    for k in range(sums_out.shape[0] // 8):
        sums_out[8 * k : 8 * k + 8, :] = row_of


def add_rows(parts):
    total = parts[0:8, :]
    for k in range(1, parts.shape[0] // 8):
        total = total + parts[8 * k : 8 * k + 8, :]
    return all_sublanes(total)


def relay(parts, sums_out):
    sums_out[...] = add_rows(parts)[0:1]


def finish(clip, up, down, *refs):
    parts, (new_out, wide) = refs[:-2], refs[-2:]
    sub = lax.broadcasted_iota(jnp.int32, (8, LANES), 0)
    lane = lax.broadcasted_iota(jnp.int32, (8, LANES), 1)
    total = parts[0][...]
    for part in parts[1:]:
        total = total + part[...]
    total = jnp.broadcast_to(total, (8, LANES))
    sums = []
    for k in range(6):
        mine = jnp.where(lane == 8 * k + sub, total, jnp.zeros_like(total))
        sums.append(jnp.broadcast_to(jnp.sum(mine, axis=1, keepdims=True), (8, LANES)))
    ratios = []
    for h in range(2):
        short, room_up, room_down = sums[3 * h : 3 * h + 3]
        raised = short >= 0
        zero = jnp.zeros_like(short)
        ratios.append(
            (jnp.where(raised, short / room_up, zero), jnp.where(raised, zero, short / room_down))
        )
    for n in range(clip.shape[0]):
        for e in range(clip.shape[1]):
            for h in range(2):
                at = (n, e, slice(8 * h, 8 * h + 8), slice(None))
                new = clip[at] + ratios[h][0] * up[at] + ratios[h][1] * down[at]
                if h == 0:
                    wide[e, pl.ds(n, 8, stride=16), :] = new
                else:
                    wide[e, 128 + n : 129 + n, :] = new[0:1]
                    wide[e, 144 + n : 145 + n, :] = new[4:5]
    for e in range(clip.shape[1]):
        new_out[:, e * LANES : (e + 1) * LANES] = wide[e]


def in_vmem(kernel, out_shape, count, scratch=(), work=0):
    spec = pl.BlockSpec(memory_space=pltpu.VMEM)
    return pl.pallas_call(
        kernel,
        out_shape=out_shape,
        in_specs=[spec] * count,
        out_specs=jax.tree.map(lambda _: spec, out_shape),
        scratch_shapes=scratch,
        cost_estimate=pl.CostEstimate(flops=work, bytes_accessed=0, transcendentals=0),
        compiler_params=pltpu.CompilerParams(vmem_limit_bytes=GRANT),
    )


def bands(field, last_out, first_out):
    last_out[...] = field[:, field.shape[1] - BAND :]
    first_out[...] = field[:, :BAND]


def line_pairs():
    count = len(ARRIVAL)
    later, earlier = [], []
    for shift in range(1, count):
        pairs = [(k, (k + shift) % count) for k in range(count)]
        later.append([(k, t) for k, t in pairs if ARRIVAL[k] > ARRIVAL[t]])
        earlier.append([(k, t) for k, t in pairs if ARRIVAL[k] < ARRIVAL[t]])
    return (later + earlier)[::-1]


PAIRS = line_pairs()


def on_device(tracer_old, air_old, air_new, dep_coord, dep_slot, fetch_list):
    _, tracers, points, e_dev = tracer_old.shape
    chunks = e_dev // LANES
    real, whole = tracer_old.dtype, jnp.int32
    field = tracer_old.reshape(tracers * points, e_dev)

    def shape(*dims, dtype=real):
        return jax.ShapeDtypeStruct(dims, dtype)

    band = shape(tracers * points, BAND)
    last, first = in_vmem(bands, (band, band), 1, work=WORK)(field)
    count = lax.axis_size(SFC)
    forward = [(i, (i + 1) % count) for i in range(count)]
    backward = [(target, source) for source, target in forward]
    left = lax.ppermute(last, SFC, forward)
    right = lax.ppermute(first, SFC, backward)
    mid = shape(points, chunks, 16, LANES)
    terms = shape(4, chunks, points, LANES)
    prepared = in_vmem(
        own_part,
        (
            shape(2, 8, LANES, dtype=whole),
            shape(points, chunks, 80, LANES, dtype=whole),
            shape(2, 8, LANES),
            terms,
            terms,
            shape(chunks, 8 * points, LANES),
            shape(chunks, points, LANES, dtype=whole),
        ),
        5,
        [
            pltpu.VMEM((chunks, tracers * points, LANES), real),
            pltpu.VMEM((chunks, 80, LANES), whole),
        ],
        WORK,
    )(field, air_old[0], dep_coord[:, 0], dep_slot[0], fetch_list[0])
    clip, up, down, sums = in_vmem(
        halo_part,
        (mid, mid, mid, shape(lax.axis_size(CUBE), LANES)),
        3 + len(prepared),
        [
            pltpu.VMEM((4, tracers * points, LANES), real),
            pltpu.VMEM((2, 80, LANES), whole),
            pltpu.VMEM((chunks, points, LANES), real),
        ],
    )(left, right, air_new[0], *prepared)
    sums = lax.all_to_all(sums, CUBE, 0, 0, tiled=True)
    sums = in_vmem(relay, shape(1, LANES), 1)(sums)
    new = in_vmem(
        finish,
        shape(tracers * points, e_dev),
        4 + len(PAIRS),
        [pltpu.VMEM((chunks, tracers * points, LANES), real)],
    )(clip, up, down, sums, *(lax.ppermute(sums, LINE, pairs) for pairs in PAIRS))
    return new.reshape(tracer_old.shape)


def solution(mesh):
    finer = Mesh(mesh.devices.reshape(8, 4, 2, 4, 4), (*SFC, *LEV))
    placed = (
        P(LEV, None, None, SFC),
        P(LEV, None, SFC),
        P(LEV, None, SFC),
        P(None, LEV, None, SFC),
        P(LEV, None, SFC),
        P(SFC, None, None),
    )
    return jax.shard_map(
        on_device, mesh=finer, in_specs=placed, out_specs=P(LEV, None, None, SFC), check_vma=False
    )
```

```python
import jax
import jax.numpy as jnp
from jax import lax
from jax.experimental import pallas as pl
from jax.experimental.pallas import tpu as pltpu
from jax.sharding import Mesh
from jax.sharding import PartitionSpec as P

BAND = 256
LANES = 128
SFC = ("sfc_0", "sfc_1")
LEV = ("lev_0", "lev_1")
PLANE = ("sfc_1", "lev_0", "lev_1")
LINE = "sfc_0"
NODES = (-1.0, -0.4472135954999579, 0.4472135954999579, 1.0)
UNROLL = 16
OWN_UNROLL = 16
STEPS = 32767.0
GRANT = 12 * 1024 * 1024
WORK = 1_000_000_000


def basis(coord):
    terms = []
    for first in range(4):
        term, scale = None, 1.0
        for other in range(4):
            if other != first:
                factor = coord - NODES[other]
                term = factor if term is None else term * factor
                scale *= NODES[first] - NODES[other]
        terms.append(term * (1.0 / scale))
    return terms


def rows(v):
    return pl.ds(v, 8, stride=16) if v < 16 else pl.ds(128 + v - 16, 8, stride=4)


def pick(table, idx):
    return jnp.take_along_axis(table, idx, axis=1, mode="promise_in_bounds")


def group_of_four(x, op):
    y = op(x, pltpu.roll(x, 7, 0))
    return op(y, pltpu.roll(y, 6, 0))


def all_sublanes(x):
    for shift in (4, 2, 1):
        x = x + pltpu.roll(x, shift, 0)
    return x


def old_mass(air_old, wide, sub):
    zero = jnp.zeros((8, LANES), jnp.float32)
    old = zero
    for c in range(wide.shape[0]):
        cols = slice(c * LANES, (c + 1) * LANES)
        for v in range(16):
            air = jnp.broadcast_to(air_old[v : v + 1, cols], (8, LANES))
            old = old + wide[c, rows(v), :] * air
    tails = []
    for t in (8, 9):
        total = zero
        for c in range(wide.shape[0]):
            cols = slice(c * LANES, (c + 1) * LANES)
            for h in (0, 8):
                at = t * 16 + h
                total = total + wide[c, at : at + 8, :] * air_old[h : h + 8, cols]
        tails.append(all_sublanes(total))
    return old, jnp.where(sub == 0, tails[0], jnp.where(sub == 4, tails[1], zero))


def fixed(x):
    return (x * STEPS + 0.5).astype(jnp.int32)


def pair(wide, c, k):
    return fixed(wide[c, rows(2 * k), :]) | (fixed(wide[c, rows(2 * k + 1), :]) << 16)


def halves(x):
    first = (x & 0xFFFF).astype(jnp.float32)
    return first, lax.shift_right_logical(x, 16).astype(jnp.float32)


def gather(pairs, along_a, along_b, stack):
    def inner(first):
        total = low = high = None
        for k in range(2):
            for q, x in enumerate(halves(pairs(first + k))):
                low = x if low is None else jnp.minimum(low, x)
                high = x if high is None else jnp.maximum(high, x)
                term = along_b[2 * k + q] * x
                total = term if total is None else total + term
        return total, low, high

    interp, low, high = inner(0)
    interp = interp * along_a[0]
    for i in range(1, 4):
        more, least, most = inner(2 * i)
        interp = interp + along_a[i] * more
        low, high = jnp.minimum(low, least), jnp.maximum(high, most)
    tail, tail_low, tail_high = inner(8)
    tail = group_of_four(tail * stack, jnp.add)
    tail_low = group_of_four(tail_low, jnp.minimum)
    tail_high = group_of_four(tail_high, jnp.maximum)
    return (interp, low, high), (tail, tail_low, tail_high)


def broadcast_row(ref, n, *at):
    return jnp.broadcast_to(ref[(*at, pl.ds(n, 1), slice(None))], (8, LANES))


def own_part(
    field, air_old, coord, slot, fetch,
    picks, own_out, old_out, along_a, along_b, stacked, slots,
    wide, table,
):
    chunks = slot.shape[1] // LANES
    points = slot.shape[0]
    sub = lax.broadcasted_iota(jnp.int32, (8, LANES), 0)
    for side, start in enumerate((chunks * LANES - BAND, 0)):
        picks[side] = jnp.broadcast_to(fetch[side : side + 1, :] - start, (8, LANES))
    for c in range(chunks):
        wide[c] = field[:, c * LANES : (c + 1) * LANES]
        slots[c] = slot[:, c * LANES : (c + 1) * LANES]
    for c in range(chunks):
        for k in range(10):
            table[c, 8 * k : 8 * k + 8, :] = pair(wide, c, k)

    def step(k, carry):
        for u in range(OWN_UNROLL):
            n = k * OWN_UNROLL + u
            for e in range(chunks):
                where = broadcast_row(slots, n, e)
                near, chunk = where & (LANES - 1), where >> 7
                masks = [chunk == c for c in range(1, chunks)]
                for k2 in range(10):
                    at = slice(8 * k2, 8 * k2 + 8)
                    x = pick(table[0, at, :], near)
                    for c, mask in enumerate(masks):
                        x = jnp.where(mask, pick(table[c + 1, at, :], near), x)
                    own_out[n, e, at, :] = x
        return carry

    lax.fori_loop(0, points // OWN_UNROLL, step, 0)
    old_out[0], old_out[1] = old_mass(air_old, wide, sub)
    terms_a = basis(coord[0])
    terms_b = basis(coord[1])
    for c in range(chunks):
        cols = slice(c * LANES, (c + 1) * LANES)
        for i in range(4):
            along_a[i, c] = terms_a[i][:, cols]
            along_b[i, c] = terms_b[i][:, cols]
            stacked[c, pl.ds(i, points, stride=8), :] = terms_a[i][:, cols]
            stacked[c, pl.ds(i + 4, points, stride=8), :] = terms_a[i][:, cols]


def halo_part(
    left, right, air_new, picks, own, old, along_a, along_b, stacked, slots,
    clip_out, up_out, down_out, sums_out,
    wide, table, airs,
):
    points, chunks = own.shape[:2]
    count = chunks * LANES
    sub = lax.broadcasted_iota(jnp.int32, (8, LANES), 0)
    lane = lax.broadcasted_iota(jnp.int32, (8, LANES), 1)
    zero = jnp.zeros((8, LANES), jnp.float32)
    for c in range(chunks):
        airs[c] = air_new[:, c * LANES : (c + 1) * LANES]
    for side, band in enumerate((left, right)):
        for c in range(2):
            wide[2 * side + c] = band[:, c * LANES : (c + 1) * LANES]
    for side in range(2):
        idx = picks[side]
        near, far = idx & (LANES - 1), idx >= LANES
        for k in range(10):
            first = pick(pair(wide, 2 * side, k), near)
            second = pick(pair(wide, 2 * side + 1, k), near)
            table[side, 8 * k : 8 * k + 8, :] = jnp.where(far, second, first)

    def group(n, e, acc):
        where = broadcast_row(slots, n, e)
        near, at_right, halo = where & (LANES - 1), where >= count + LANES, where >= count

        def pairs(k):
            at = slice(8 * k, 8 * k + 8)
            x = jnp.where(at_right, pick(table[1, at, :], near), pick(table[0, at, :], near))
            return jnp.where(halo, x, own[n, e, at, :])

        row_a, row_b = (
            [broadcast_row(ref, n, i, e) for i in range(4)] for ref in (along_a, along_b)
        )
        parts = gather(pairs, row_a, row_b, stacked[e, pl.ds(pl.multiple_of(8 * n, 8), 8), :])
        air = broadcast_row(airs, n, e)
        acc = list(acc)
        for h, (f, lo, hi) in enumerate(parts):
            at = (n, e, slice(8 * h, 8 * h + 8), slice(None))
            f = jnp.minimum(jnp.maximum(f, lo), hi)
            f, up, down = f * (1.0 / STEPS), (hi - f) * (1.0 / STEPS), (f - lo) * (1.0 / STEPS)
            clip_out[at], up_out[at], down_out[at] = f, up, down
            acc[3 * h] = acc[3 * h] - air * f
            acc[3 * h + 1] = acc[3 * h + 1] + air * up
            acc[3 * h + 2] = acc[3 * h + 2] + air * down
        return tuple(acc)

    def step(k, acc):
        for u in range(UNROLL):
            for e in range(chunks):
                acc = group(k * UNROLL + u, e, acc)
        return acc

    acc = lax.fori_loop(0, points // UNROLL, step, (old[0], zero, zero, old[1], zero, zero))
    row_of = zero
    for k in range(6):
        total = jnp.broadcast_to(jnp.sum(acc[k], axis=1, keepdims=True), (8, LANES))
        keep = lane == 8 * k + sub
        if k >= 3:
            keep = keep & ((sub & 3) == 0)
        row_of = row_of + jnp.where(keep, total, zero)
    row_of = all_sublanes(row_of)
    for k in range(sums_out.shape[0] // 8):
        sums_out[8 * k : 8 * k + 8, :] = row_of


def add_rows(parts):
    total = parts[0:8, :]
    for k in range(1, parts.shape[0] // 8):
        total = total + parts[8 * k : 8 * k + 8, :]
    return all_sublanes(total)


def relay(parts, sums_out):
    total = add_rows(parts)
    for k in range(sums_out.shape[0] // 8):
        sums_out[8 * k : 8 * k + 8, :] = total


def finish(parts, clip, up, down, new_out, wide, sent):
    sub = lax.broadcasted_iota(jnp.int32, (8, LANES), 0)
    lane = lax.broadcasted_iota(jnp.int32, (8, LANES), 1)
    total = add_rows(parts)
    sums = []
    for k in range(6):
        mine = jnp.where(lane == 8 * k + sub, total, jnp.zeros_like(total))
        sums.append(jnp.broadcast_to(jnp.sum(mine, axis=1, keepdims=True), (8, LANES)))
    ratios = []
    for h in range(2):
        short, room_up, room_down = sums[3 * h : 3 * h + 3]
        raised = short >= 0
        zero = jnp.zeros_like(short)
        ratios.append(
            (jnp.where(raised, short / room_up, zero), jnp.where(raised, zero, short / room_down))
        )
    copies = []
    for e in range(clip.shape[1]):
        for n in range(clip.shape[0]):
            for h in range(2):
                at = (n, e, slice(8 * h, 8 * h + 8), slice(None))
                new = clip[at] + ratios[h][0] * up[at] + ratios[h][1] * down[at]
                if h == 0:
                    wide[e, pl.ds(n, 8, stride=16), :] = new
                else:
                    wide[e, 128 + n : 129 + n, :] = new[0:1]
                    wide[e, 144 + n : 145 + n, :] = new[4:5]
        copy = pltpu.make_async_copy(wide.at[e], new_out.at[:, pl.ds(e * LANES, LANES)], sent.at[e])
        copy.start()
        copies.append(copy)
    for copy in copies:
        copy.wait()


def in_vmem(kernel, out_shape, count, scratch=(), work=0, out_space=pltpu.VMEM):
    spec = pl.BlockSpec(memory_space=pltpu.VMEM)
    return pl.pallas_call(
        kernel,
        out_shape=out_shape,
        in_specs=[spec] * count,
        out_specs=jax.tree.map(lambda _: pl.BlockSpec(memory_space=out_space), out_shape),
        scratch_shapes=scratch,
        cost_estimate=pl.CostEstimate(flops=work, bytes_accessed=0, transcendentals=0),
        compiler_params=pltpu.CompilerParams(vmem_limit_bytes=GRANT),
    )


def bands(field, last_out, first_out):
    last_out[...] = field[:, field.shape[1] - BAND :]
    first_out[...] = field[:, :BAND]


def on_device(tracer_old, air_old, air_new, dep_coord, dep_slot, fetch_list):
    _, tracers, points, e_dev = tracer_old.shape
    chunks = e_dev // LANES
    real, whole = tracer_old.dtype, jnp.int32
    field = tracer_old.reshape(tracers * points, e_dev)

    def shape(*dims, dtype=real):
        return jax.ShapeDtypeStruct(dims, dtype)

    band = shape(tracers * points, BAND)
    last, first = in_vmem(bands, (band, band), 1, work=WORK)(field)
    count = lax.axis_size(SFC)
    forward = [(i, (i + 1) % count) for i in range(count)]
    backward = [(target, source) for source, target in forward]
    left = lax.ppermute(last, SFC, forward)
    right = lax.ppermute(first, SFC, backward)
    mid = shape(points, chunks, 16, LANES)
    plane, line = lax.axis_size(PLANE), lax.axis_size(LINE)
    terms = shape(4, chunks, points, LANES)
    prepared = in_vmem(
        own_part,
        (
            shape(2, 8, LANES, dtype=whole),
            shape(points, chunks, 80, LANES, dtype=whole),
            shape(2, 8, LANES),
            terms,
            terms,
            shape(chunks, 8 * points, LANES),
            shape(chunks, points, LANES, dtype=whole),
        ),
        5,
        [
            pltpu.VMEM((chunks, tracers * points, LANES), real),
            pltpu.VMEM((chunks, 80, LANES), whole),
        ],
        WORK,
    )(field, air_old[0], dep_coord[:, 0], dep_slot[0], fetch_list[0])
    clip, up, down, sums = in_vmem(
        halo_part,
        (mid, mid, mid, shape(plane, LANES)),
        3 + len(prepared),
        [
            pltpu.VMEM((4, tracers * points, LANES), real),
            pltpu.VMEM((2, 80, LANES), whole),
            pltpu.VMEM((chunks, points, LANES), real),
        ],
    )(left, right, air_new[0], *prepared)
    sums = lax.all_to_all(sums, PLANE, 0, 0, tiled=True)
    sums = in_vmem(relay, shape(line, LANES), 1)(sums)
    sums = lax.all_to_all(sums, LINE, 0, 0, tiled=True)
    new = in_vmem(
        finish,
        shape(tracers * points, e_dev),
        4,
        [
            pltpu.VMEM((chunks, tracers * points, LANES), real),
            pltpu.SemaphoreType.DMA((chunks,)),
        ],
        out_space=pl.ANY,
    )(sums, clip, up, down)
    return new.reshape(tracer_old.shape)


def solution(mesh):
    finer = Mesh(mesh.devices.reshape(32, 2, 4, 4), ("sfc_0", "sfc_1", "lev_0", "lev_1"))
    placed = (
        P(LEV, None, None, SFC),
        P(LEV, None, SFC),
        P(LEV, None, SFC),
        P(None, LEV, None, SFC),
        P(LEV, None, SFC),
        P(SFC, None, None),
    )
    return jax.shard_map(
        on_device, mesh=finer, in_specs=placed, out_specs=P(LEV, None, None, SFC), check_vma=False
    )
```

```python
import jax
import jax.numpy as jnp
from jax import lax
from jax.experimental import pallas as pl
from jax.experimental.pallas import tpu as pltpu
from jax.sharding import Mesh
from jax.sharding import PartitionSpec as P

BAND = 256
LANES = 128
SFC = ("sfc_0", "sfc_1")
LEV = ("lev_0", "lev_1")
PLANE = ("sfc_1", "lev_0", "lev_1")
LINE = "sfc_0"
NODES = (-1.0, -0.4472135954999579, 0.4472135954999579, 1.0)
UNROLL = 16
OWN_UNROLL = 16
STEPS = 32767.0
GRANT = 12 * 1024 * 1024
WORK = 1_000_000_000


def basis(coord):
    terms = []
    for first in range(4):
        term, scale = None, 1.0
        for other in range(4):
            if other != first:
                factor = coord - NODES[other]
                term = factor if term is None else term * factor
                scale *= NODES[first] - NODES[other]
        terms.append(term * (1.0 / scale))
    return terms


def rows(v):
    return pl.ds(v, 8, stride=16) if v < 16 else pl.ds(128 + v - 16, 8, stride=4)


def pick(table, idx):
    return jnp.take_along_axis(table, idx, axis=1, mode="promise_in_bounds")


def group_of_four(x, op):
    y = op(x, pltpu.roll(x, 7, 0))
    return op(y, pltpu.roll(y, 6, 0))


def all_sublanes(x):
    for shift in (4, 2, 1):
        x = x + pltpu.roll(x, shift, 0)
    return x


def old_mass(air_old, wide, sub):
    zero = jnp.zeros((8, LANES), jnp.float32)
    old = zero
    for c in range(wide.shape[0]):
        cols = slice(c * LANES, (c + 1) * LANES)
        for v in range(16):
            air = jnp.broadcast_to(air_old[v : v + 1, cols], (8, LANES))
            old = old + wide[c, rows(v), :] * air
    tails = []
    for t in (8, 9):
        total = zero
        for c in range(wide.shape[0]):
            cols = slice(c * LANES, (c + 1) * LANES)
            for h in (0, 8):
                at = t * 16 + h
                total = total + wide[c, at : at + 8, :] * air_old[h : h + 8, cols]
        tails.append(all_sublanes(total))
    return old, jnp.where(sub == 0, tails[0], jnp.where(sub == 4, tails[1], zero))


def fixed(x):
    return (x * STEPS + 0.5).astype(jnp.int32)


def pair(wide, c, k):
    return fixed(wide[c, rows(2 * k), :]) | (fixed(wide[c, rows(2 * k + 1), :]) << 16)


def halves(x):
    first = (x & 0xFFFF).astype(jnp.float32)
    return first, lax.shift_right_logical(x, 16).astype(jnp.float32)


def gather(pairs, along_a, along_b, stack):
    def inner(first):
        total = low = high = None
        for k in range(2):
            for q, x in enumerate(halves(pairs(first + k))):
                low = x if low is None else jnp.minimum(low, x)
                high = x if high is None else jnp.maximum(high, x)
                term = along_b[2 * k + q] * x
                total = term if total is None else total + term
        return total, low, high

    interp, low, high = inner(0)
    interp = interp * along_a[0]
    for i in range(1, 4):
        more, least, most = inner(2 * i)
        interp = interp + along_a[i] * more
        low, high = jnp.minimum(low, least), jnp.maximum(high, most)
    tail, tail_low, tail_high = inner(8)
    tail = group_of_four(tail * stack, jnp.add)
    tail_low = group_of_four(tail_low, jnp.minimum)
    tail_high = group_of_four(tail_high, jnp.maximum)
    return (interp, low, high), (tail, tail_low, tail_high)


def broadcast_row(ref, n, *at):
    return jnp.broadcast_to(ref[(*at, pl.ds(n, 1), slice(None))], (8, LANES))


def own_part(
    field, air_old, coord, slot, fetch,
    picks, own_out, old_out, along_a, along_b, stacked, slots,
    wide, table,
):
    chunks = slot.shape[1] // LANES
    points = slot.shape[0]
    sub = lax.broadcasted_iota(jnp.int32, (8, LANES), 0)
    for side, start in enumerate((chunks * LANES - BAND, 0)):
        picks[side] = jnp.broadcast_to(fetch[side : side + 1, :] - start, (8, LANES))
    for c in range(chunks):
        wide[c] = field[:, c * LANES : (c + 1) * LANES]
        slots[c] = slot[:, c * LANES : (c + 1) * LANES]
    for c in range(chunks):
        for k in range(10):
            table[c, 8 * k : 8 * k + 8, :] = pair(wide, c, k)

    def step(k, carry):
        for u in range(OWN_UNROLL):
            n = k * OWN_UNROLL + u
            for e in range(chunks):
                where = broadcast_row(slots, n, e)
                near, chunk = where & (LANES - 1), where >> 7
                masks = [chunk == c for c in range(1, chunks)]
                for k2 in range(10):
                    at = slice(8 * k2, 8 * k2 + 8)
                    x = pick(table[0, at, :], near)
                    for c, mask in enumerate(masks):
                        x = jnp.where(mask, pick(table[c + 1, at, :], near), x)
                    own_out[n, e, at, :] = x
        return carry

    lax.fori_loop(0, points // OWN_UNROLL, step, 0)
    old_out[0], old_out[1] = old_mass(air_old, wide, sub)
    terms_a = basis(coord[0])
    terms_b = basis(coord[1])
    for c in range(chunks):
        cols = slice(c * LANES, (c + 1) * LANES)
        for i in range(4):
            along_a[i, c] = terms_a[i][:, cols]
            along_b[i, c] = terms_b[i][:, cols]
            stacked[c, pl.ds(i, points, stride=8), :] = terms_a[i][:, cols]
            stacked[c, pl.ds(i + 4, points, stride=8), :] = terms_a[i][:, cols]


def halo_part(
    right, left, air_new, picks, own, old, along_a, along_b, stacked, slots,
    clip_out, up_out, down_out, sums_out,
    wide, table, airs,
):
    points, chunks = own.shape[:2]
    count = chunks * LANES
    sub = lax.broadcasted_iota(jnp.int32, (8, LANES), 0)
    lane = lax.broadcasted_iota(jnp.int32, (8, LANES), 1)
    zero = jnp.zeros((8, LANES), jnp.float32)
    for c in range(chunks):
        airs[c] = air_new[:, c * LANES : (c + 1) * LANES]
    for side, band in enumerate((left, right)):
        for c in range(2):
            wide[2 * side + c] = band[:, c * LANES : (c + 1) * LANES]
    for side in range(2):
        idx = picks[side]
        near, far = idx & (LANES - 1), idx >= LANES
        for k in range(10):
            first = pick(pair(wide, 2 * side, k), near)
            second = pick(pair(wide, 2 * side + 1, k), near)
            table[side, 8 * k : 8 * k + 8, :] = jnp.where(far, second, first)

    def group(n, e, acc):
        where = broadcast_row(slots, n, e)
        near, at_right, halo = where & (LANES - 1), where >= count + LANES, where >= count

        def pairs(k):
            at = slice(8 * k, 8 * k + 8)
            x = jnp.where(at_right, pick(table[1, at, :], near), pick(table[0, at, :], near))
            return jnp.where(halo, x, own[n, e, at, :])

        row_a, row_b = (
            [broadcast_row(ref, n, i, e) for i in range(4)] for ref in (along_a, along_b)
        )
        parts = gather(pairs, row_a, row_b, stacked[e, pl.ds(pl.multiple_of(8 * n, 8), 8), :])
        air = broadcast_row(airs, n, e)
        acc = list(acc)
        for h, (f, lo, hi) in enumerate(parts):
            at = (n, e, slice(8 * h, 8 * h + 8), slice(None))
            f = jnp.minimum(jnp.maximum(f, lo), hi)
            f, up, down = f * (1.0 / STEPS), (hi - f) * (1.0 / STEPS), (f - lo) * (1.0 / STEPS)
            clip_out[at], up_out[at], down_out[at] = f, up, down
            acc[3 * h] = acc[3 * h] - air * f
            acc[3 * h + 1] = acc[3 * h + 1] + air * up
            acc[3 * h + 2] = acc[3 * h + 2] + air * down
        return tuple(acc)

    def step(k, acc):
        for u in range(UNROLL):
            for e in range(chunks):
                acc = group(k * UNROLL + u, e, acc)
        return acc

    acc = lax.fori_loop(0, points // UNROLL, step, (old[0], zero, zero, old[1], zero, zero))
    row_of = zero
    for k in range(6):
        total = jnp.broadcast_to(jnp.sum(acc[k], axis=1, keepdims=True), (8, LANES))
        keep = lane == 8 * k + sub
        if k >= 3:
            keep = keep & ((sub & 3) == 0)
        row_of = row_of + jnp.where(keep, total, zero)
    row_of = all_sublanes(row_of)
    for k in range(sums_out.shape[0] // 8):
        sums_out[8 * k : 8 * k + 8, :] = row_of


def add_rows(parts):
    total = parts[0:8, :]
    for k in range(1, parts.shape[0] // 8):
        total = total + parts[8 * k : 8 * k + 8, :]
    return all_sublanes(total)


def relay(parts, sums_out):
    total = add_rows(parts)
    for k in range(sums_out.shape[0] // 8):
        sums_out[8 * k : 8 * k + 8, :] = total


def finish(parts, clip, up, down, new_out, wide, sent):
    sub = lax.broadcasted_iota(jnp.int32, (8, LANES), 0)
    lane = lax.broadcasted_iota(jnp.int32, (8, LANES), 1)
    total = add_rows(parts)
    sums = []
    for k in range(6):
        mine = jnp.where(lane == 8 * k + sub, total, jnp.zeros_like(total))
        sums.append(jnp.broadcast_to(jnp.sum(mine, axis=1, keepdims=True), (8, LANES)))
    ratios = []
    for h in range(2):
        short, room_up, room_down = sums[3 * h : 3 * h + 3]
        raised = short >= 0
        zero = jnp.zeros_like(short)
        ratios.append(
            (jnp.where(raised, short / room_up, zero), jnp.where(raised, zero, short / room_down))
        )
    copies = []
    for e in range(clip.shape[1]):
        for n in range(clip.shape[0]):
            for h in range(2):
                at = (n, e, slice(8 * h, 8 * h + 8), slice(None))
                new = clip[at] + ratios[h][0] * up[at] + ratios[h][1] * down[at]
                if h == 0:
                    wide[e, pl.ds(n, 8, stride=16), :] = new
                else:
                    wide[e, 128 + n : 129 + n, :] = new[0:1]
                    wide[e, 144 + n : 145 + n, :] = new[4:5]
        copy = pltpu.make_async_copy(wide.at[e], new_out.at[:, pl.ds(e * LANES, LANES)], sent.at[e])
        copy.start()
        copies.append(copy)
    for copy in copies:
        copy.wait()


def in_vmem(kernel, out_shape, count, scratch=(), work=0, out_space=pltpu.VMEM):
    spec = pl.BlockSpec(memory_space=pltpu.VMEM)
    return pl.pallas_call(
        kernel,
        out_shape=out_shape,
        in_specs=[spec] * count,
        out_specs=jax.tree.map(lambda _: pl.BlockSpec(memory_space=out_space), out_shape),
        scratch_shapes=scratch,
        cost_estimate=pl.CostEstimate(flops=work, bytes_accessed=0, transcendentals=0),
        compiler_params=pltpu.CompilerParams(vmem_limit_bytes=GRANT),
    )


def bands(field, last_out, first_out):
    last_out[...] = field[:, field.shape[1] - BAND :]
    first_out[...] = field[:, :BAND]


def on_device(tracer_old, air_old, air_new, dep_coord, dep_slot, fetch_list):
    _, tracers, points, e_dev = tracer_old.shape
    chunks = e_dev // LANES
    real, whole = tracer_old.dtype, jnp.int32
    field = tracer_old.reshape(tracers * points, e_dev)

    def shape(*dims, dtype=real):
        return jax.ShapeDtypeStruct(dims, dtype)

    band = shape(tracers * points, BAND)
    last, first = in_vmem(bands, (band, band), 1, work=WORK)(field)
    count = lax.axis_size(SFC)
    forward = [(i, (i + 1) % count) for i in range(count)]
    backward = [(target, source) for source, target in forward]
    right = lax.ppermute(first, SFC, backward)
    left = lax.ppermute(last, SFC, forward)
    mid = shape(points, chunks, 16, LANES)
    plane, line = lax.axis_size(PLANE), lax.axis_size(LINE)
    terms = shape(4, chunks, points, LANES)
    prepared = in_vmem(
        own_part,
        (
            shape(2, 8, LANES, dtype=whole),
            shape(points, chunks, 80, LANES, dtype=whole),
            shape(2, 8, LANES),
            terms,
            terms,
            shape(chunks, 8 * points, LANES),
            shape(chunks, points, LANES, dtype=whole),
        ),
        5,
        [
            pltpu.VMEM((chunks, tracers * points, LANES), real),
            pltpu.VMEM((chunks, 80, LANES), whole),
        ],
        WORK,
    )(field, air_old[0], dep_coord[:, 0], dep_slot[0], fetch_list[0])
    clip, up, down, sums = in_vmem(
        halo_part,
        (mid, mid, mid, shape(line, LANES)),
        3 + len(prepared),
        [
            pltpu.VMEM((4, tracers * points, LANES), real),
            pltpu.VMEM((2, 80, LANES), whole),
            pltpu.VMEM((chunks, points, LANES), real),
        ],
    )(right, left, air_new[0], *prepared)
    sums = lax.all_to_all(sums, LINE, 0, 0, tiled=True)
    sums = in_vmem(relay, shape(plane, LANES), 1)(sums)
    sums = lax.all_to_all(sums, PLANE, 0, 0, tiled=True)
    new = in_vmem(
        finish,
        shape(tracers * points, e_dev),
        4,
        [
            pltpu.VMEM((chunks, tracers * points, LANES), real),
            pltpu.SemaphoreType.DMA((chunks,)),
        ],
        out_space=pl.ANY,
    )(sums, clip, up, down)
    return new.reshape(tracer_old.shape)


def solution(mesh):
    finer = Mesh(mesh.devices.reshape(32, 2, 4, 4), ("sfc_0", "sfc_1", "lev_0", "lev_1"))
    placed = (
        P(LEV, None, None, SFC),
        P(LEV, None, SFC),
        P(LEV, None, SFC),
        P(None, LEV, None, SFC),
        P(LEV, None, SFC),
        P(SFC, None, None),
    )
    return jax.shard_map(
        on_device, mesh=finer, in_specs=placed, out_specs=P(LEV, None, None, SFC), check_vma=False
    )
```

```python
import jax
import jax.numpy as jnp
from jax import lax
from jax.experimental import pallas as pl
from jax.experimental.pallas import tpu as pltpu
from jax.sharding import Mesh
from jax.sharding import PartitionSpec as P

BAND = 256
LANES = 128
SFC = ("sfc_0", "sfc_1")
LEV = ("lev_0", "lev_1")
PLANE = ("sfc_1", "lev_0", "lev_1")
LINE = "sfc_0"
NODES = (-1.0, -0.4472135954999579, 0.4472135954999579, 1.0)
UNROLL = 16
OWN_UNROLL = 16
STEPS = 32767.0
GRANT = 12 * 1024 * 1024
WORK = 1_000_000_000


def basis(coord):
    terms = []
    for first in range(4):
        term, scale = None, 1.0
        for other in range(4):
            if other != first:
                factor = coord - NODES[other]
                term = factor if term is None else term * factor
                scale *= NODES[first] - NODES[other]
        terms.append(term * (1.0 / scale))
    return terms


def rows(v):
    return pl.ds(v, 8, stride=16) if v < 16 else pl.ds(128 + v - 16, 8, stride=4)


def pick(table, idx):
    return jnp.take_along_axis(table, idx, axis=1, mode="promise_in_bounds")


def group_of_four(x, op):
    y = op(x, pltpu.roll(x, 7, 0))
    return op(y, pltpu.roll(y, 6, 0))


def all_sublanes(x):
    for shift in (4, 2, 1):
        x = x + pltpu.roll(x, shift, 0)
    return x


def old_mass(air_old, wide, sub):
    zero = jnp.zeros((8, LANES), jnp.float32)
    old = zero
    for c in range(wide.shape[0]):
        cols = slice(c * LANES, (c + 1) * LANES)
        for v in range(16):
            air = jnp.broadcast_to(air_old[v : v + 1, cols], (8, LANES))
            old = old + wide[c, rows(v), :] * air
    tails = []
    for t in (8, 9):
        total = zero
        for c in range(wide.shape[0]):
            cols = slice(c * LANES, (c + 1) * LANES)
            for h in (0, 8):
                at = t * 16 + h
                total = total + wide[c, at : at + 8, :] * air_old[h : h + 8, cols]
        tails.append(all_sublanes(total))
    return old, jnp.where(sub == 0, tails[0], jnp.where(sub == 4, tails[1], zero))


def fixed(x):
    return (x * STEPS + 0.5).astype(jnp.int32)


def pair(wide, c, k):
    return fixed(wide[c, rows(2 * k), :]) | (fixed(wide[c, rows(2 * k + 1), :]) << 16)


def halves(x):
    first = (x & 0xFFFF).astype(jnp.float32)
    return first, lax.shift_right_logical(x, 16).astype(jnp.float32)


def gather(pairs, along_a, along_b, stack):
    def inner(first):
        total = low = high = None
        for k in range(2):
            for q, x in enumerate(halves(pairs(first + k))):
                low = x if low is None else jnp.minimum(low, x)
                high = x if high is None else jnp.maximum(high, x)
                term = along_b[2 * k + q] * x
                total = term if total is None else total + term
        return total, low, high

    interp, low, high = inner(0)
    interp = interp * along_a[0]
    for i in range(1, 4):
        more, least, most = inner(2 * i)
        interp = interp + along_a[i] * more
        low, high = jnp.minimum(low, least), jnp.maximum(high, most)
    tail, tail_low, tail_high = inner(8)
    tail = group_of_four(tail * stack, jnp.add)
    tail_low = group_of_four(tail_low, jnp.minimum)
    tail_high = group_of_four(tail_high, jnp.maximum)
    return (interp, low, high), (tail, tail_low, tail_high)


def broadcast_row(ref, n, *at):
    return jnp.broadcast_to(ref[(*at, pl.ds(n, 1), slice(None))], (8, LANES))


def own_part(
    field, air_old, coord, slot, fetch,
    picks, own_out, old_out, along_a, along_b, stacked, slots,
    wide, table,
):
    chunks = slot.shape[1] // LANES
    points = slot.shape[0]
    sub = lax.broadcasted_iota(jnp.int32, (8, LANES), 0)
    for side, start in enumerate((chunks * LANES - BAND, 0)):
        picks[side] = jnp.broadcast_to(fetch[side : side + 1, :] - start, (8, LANES))
    for c in range(chunks):
        wide[c] = field[:, c * LANES : (c + 1) * LANES]
        slots[c] = slot[:, c * LANES : (c + 1) * LANES]
    for c in range(chunks):
        for k in range(10):
            table[c, 8 * k : 8 * k + 8, :] = pair(wide, c, k)

    def step(k, carry):
        for u in range(OWN_UNROLL):
            n = k * OWN_UNROLL + u
            for e in range(chunks):
                where = broadcast_row(slots, n, e)
                near, chunk = where & (LANES - 1), where >> 7
                masks = [chunk == c for c in range(1, chunks)]
                for k2 in range(10):
                    at = slice(8 * k2, 8 * k2 + 8)
                    x = pick(table[0, at, :], near)
                    for c, mask in enumerate(masks):
                        x = jnp.where(mask, pick(table[c + 1, at, :], near), x)
                    own_out[n, e, at, :] = x
        return carry

    lax.fori_loop(0, points // OWN_UNROLL, step, 0)
    old_out[0], old_out[1] = old_mass(air_old, wide, sub)
    terms_a = basis(coord[0])
    terms_b = basis(coord[1])
    for c in range(chunks):
        cols = slice(c * LANES, (c + 1) * LANES)
        for i in range(4):
            along_a[i, c] = terms_a[i][:, cols]
            along_b[i, c] = terms_b[i][:, cols]
            stacked[c, pl.ds(i, points, stride=8), :] = terms_a[i][:, cols]
            stacked[c, pl.ds(i + 4, points, stride=8), :] = terms_a[i][:, cols]


def halo_part(
    right, left, air_new, picks, own, old, along_a, along_b, stacked, slots,
    clip_out, up_out, down_out, sums_out,
    wide, table, airs,
):
    points, chunks = own.shape[:2]
    count = chunks * LANES
    sub = lax.broadcasted_iota(jnp.int32, (8, LANES), 0)
    lane = lax.broadcasted_iota(jnp.int32, (8, LANES), 1)
    zero = jnp.zeros((8, LANES), jnp.float32)
    for c in range(chunks):
        airs[c] = air_new[:, c * LANES : (c + 1) * LANES]
    for side, band in enumerate((left, right)):
        for c in range(2):
            wide[2 * side + c] = band[:, c * LANES : (c + 1) * LANES]
    for side in range(2):
        idx = picks[side]
        near, far = idx & (LANES - 1), idx >= LANES
        for k in range(10):
            first = pick(pair(wide, 2 * side, k), near)
            second = pick(pair(wide, 2 * side + 1, k), near)
            table[side, 8 * k : 8 * k + 8, :] = jnp.where(far, second, first)

    def group(n, e, acc):
        where = broadcast_row(slots, n, e)
        near, at_right, halo = where & (LANES - 1), where >= count + LANES, where >= count

        def pairs(k):
            at = slice(8 * k, 8 * k + 8)
            x = jnp.where(at_right, pick(table[1, at, :], near), pick(table[0, at, :], near))
            return jnp.where(halo, x, own[n, e, at, :])

        row_a, row_b = (
            [broadcast_row(ref, n, i, e) for i in range(4)] for ref in (along_a, along_b)
        )
        parts = gather(pairs, row_a, row_b, stacked[e, pl.ds(pl.multiple_of(8 * n, 8), 8), :])
        air = broadcast_row(airs, n, e)
        acc = list(acc)
        for h, (f, lo, hi) in enumerate(parts):
            at = (n, e, slice(8 * h, 8 * h + 8), slice(None))
            f = jnp.minimum(jnp.maximum(f, lo), hi)
            f, up, down = f * (1.0 / STEPS), (hi - f) * (1.0 / STEPS), (f - lo) * (1.0 / STEPS)
            clip_out[at], up_out[at], down_out[at] = f, up, down
            acc[3 * h] = acc[3 * h] - air * f
            acc[3 * h + 1] = acc[3 * h + 1] + air * up
            acc[3 * h + 2] = acc[3 * h + 2] + air * down
        return tuple(acc)

    def step(k, acc):
        for u in range(UNROLL):
            for e in range(chunks):
                acc = group(k * UNROLL + u, e, acc)
        return acc

    acc = lax.fori_loop(0, points // UNROLL, step, (old[0], zero, zero, old[1], zero, zero))
    row_of = zero
    for k in range(6):
        total = jnp.broadcast_to(jnp.sum(acc[k], axis=1, keepdims=True), (8, LANES))
        keep = lane == 8 * k + sub
        if k >= 3:
            keep = keep & ((sub & 3) == 0)
        row_of = row_of + jnp.where(keep, total, zero)
    row_of = all_sublanes(row_of)
    for k in range(sums_out.shape[0] // 8):
        sums_out[8 * k : 8 * k + 8, :] = row_of


def add_rows(parts):
    total = parts[0:8, :]
    for k in range(1, parts.shape[0] // 8):
        total = total + parts[8 * k : 8 * k + 8, :]
    return all_sublanes(total)


def relay(parts, sums_out):
    total = add_rows(parts)
    for k in range(sums_out.shape[0] // 8):
        sums_out[8 * k : 8 * k + 8, :] = total


def finish(parts, clip, up, down, new_out, wide, sent):
    sub = lax.broadcasted_iota(jnp.int32, (8, LANES), 0)
    lane = lax.broadcasted_iota(jnp.int32, (8, LANES), 1)
    total = add_rows(parts)
    sums = []
    for k in range(6):
        mine = jnp.where(lane == 8 * k + sub, total, jnp.zeros_like(total))
        sums.append(jnp.broadcast_to(jnp.sum(mine, axis=1, keepdims=True), (8, LANES)))
    ratios = []
    for h in range(2):
        short, room_up, room_down = sums[3 * h : 3 * h + 3]
        raised = short >= 0
        zero = jnp.zeros_like(short)
        ratios.append(
            (jnp.where(raised, short / room_up, zero), jnp.where(raised, zero, short / room_down))
        )
    copies = []
    for e in range(clip.shape[1]):
        for n in range(clip.shape[0]):
            for h in range(2):
                at = (n, e, slice(8 * h, 8 * h + 8), slice(None))
                new = clip[at] + ratios[h][0] * up[at] + ratios[h][1] * down[at]
                if h == 0:
                    wide[e, pl.ds(n, 8, stride=16), :] = new
                else:
                    wide[e, 128 + n : 129 + n, :] = new[0:1]
                    wide[e, 144 + n : 145 + n, :] = new[4:5]
        copy = pltpu.make_async_copy(wide.at[e], new_out.at[:, pl.ds(e * LANES, LANES)], sent.at[e])
        copy.start()
        copies.append(copy)
    for copy in copies:
        copy.wait()


def in_vmem(kernel, out_shape, count, scratch=(), work=0, out_space=pltpu.VMEM):
    spec = pl.BlockSpec(memory_space=pltpu.VMEM)
    return pl.pallas_call(
        kernel,
        out_shape=out_shape,
        in_specs=[spec] * count,
        out_specs=jax.tree.map(lambda _: pl.BlockSpec(memory_space=out_space), out_shape),
        scratch_shapes=scratch,
        cost_estimate=pl.CostEstimate(flops=work, bytes_accessed=0, transcendentals=0),
        compiler_params=pltpu.CompilerParams(vmem_limit_bytes=GRANT),
    )


def bands(field, last_out, first_out):
    last_out[...] = field[:, field.shape[1] - BAND :]
    first_out[...] = field[:, :BAND]


def on_device(tracer_old, air_old, air_new, dep_coord, dep_slot, fetch_list):
    _, tracers, points, e_dev = tracer_old.shape
    chunks = e_dev // LANES
    real, whole = tracer_old.dtype, jnp.int32
    field = tracer_old.reshape(tracers * points, e_dev)

    def shape(*dims, dtype=real):
        return jax.ShapeDtypeStruct(dims, dtype)

    band = shape(tracers * points, BAND)
    last, first = in_vmem(bands, (band, band), 1, work=WORK)(field)
    count = lax.axis_size(SFC)
    forward = [(i, (i + 1) % count) for i in range(count)]
    backward = [(target, source) for source, target in forward]
    right = lax.ppermute(first, SFC, backward)
    left = lax.ppermute(last, SFC, forward)
    mid = shape(points, chunks, 16, LANES)
    plane, line = lax.axis_size(PLANE), lax.axis_size(LINE)
    terms = shape(4, chunks, points, LANES)
    prepared = in_vmem(
        own_part,
        (
            shape(2, 8, LANES, dtype=whole),
            shape(points, chunks, 80, LANES, dtype=whole),
            shape(2, 8, LANES),
            terms,
            terms,
            shape(chunks, 8 * points, LANES),
            shape(chunks, points, LANES, dtype=whole),
        ),
        5,
        [
            pltpu.VMEM((chunks, tracers * points, LANES), real),
            pltpu.VMEM((chunks, 80, LANES), whole),
        ],
        WORK,
    )(field, air_old[0], dep_coord[:, 0], dep_slot[0], fetch_list[0])
    clip, up, down, sums = in_vmem(
        halo_part,
        (mid, mid, mid, shape(plane, LANES)),
        3 + len(prepared),
        [
            pltpu.VMEM((4, tracers * points, LANES), real),
            pltpu.VMEM((2, 80, LANES), whole),
            pltpu.VMEM((chunks, points, LANES), real),
        ],
    )(right, left, air_new[0], *prepared)
    sums = lax.all_to_all(sums, PLANE, 0, 0, tiled=True)
    sums = in_vmem(relay, shape(line, LANES), 1)(sums)
    sums = lax.all_to_all(sums, LINE, 0, 0, tiled=True)
    new = in_vmem(
        finish,
        shape(tracers * points, e_dev),
        4,
        [
            pltpu.VMEM((chunks, tracers * points, LANES), real),
            pltpu.SemaphoreType.DMA((chunks,)),
        ],
        out_space=pl.ANY,
    )(sums, clip, up, down)
    return new.reshape(tracer_old.shape)


def solution(mesh):
    finer = Mesh(mesh.devices.reshape(32, 2, 4, 4), ("sfc_0", "sfc_1", "lev_0", "lev_1"))
    placed = (
        P(LEV, None, None, SFC),
        P(LEV, None, SFC),
        P(LEV, None, SFC),
        P(None, LEV, None, SFC),
        P(LEV, None, SFC),
        P(SFC, None, None),
    )
    return jax.shard_map(
        on_device, mesh=finer, in_specs=placed, out_specs=P(LEV, None, None, SFC), check_vma=False
    )
```

```python
import jax
import jax.numpy as jnp
from jax import lax
from jax.experimental import pallas as pl
from jax.experimental.pallas import tpu as pltpu
from jax.sharding import Mesh
from jax.sharding import PartitionSpec as P

BAND = 256
LANES = 128
SFC = ("sfc_0", "sfc_1")
LEV = ("lev_0", "lev_1")
PLANE = ("sfc_1", "lev_0", "lev_1")
LINE = "sfc_0"
NODES = (-1.0, -0.4472135954999579, 0.4472135954999579, 1.0)
REGISTERS = 20
UNROLL = 16
OWN_UNROLL = 16
GRANT = 12 * 1024 * 1024
WORK = 1_000_000_000
LOAD = 10_000_000_000


def basis(coord):
    terms = []
    for first in range(4):
        term, scale = None, 1.0
        for other in range(4):
            if other != first:
                factor = coord - NODES[other]
                term = factor if term is None else term * factor
                scale *= NODES[first] - NODES[other]
        terms.append(term * (1.0 / scale))
    return terms


def rows(v):
    return pl.ds(v, 8, stride=16) if v < 16 else pl.ds(128 + v - 16, 8, stride=4)


def pick(table, idx):
    return jnp.take_along_axis(table, idx, axis=1, mode="promise_in_bounds")


def group_of_four(x, op):
    y = op(x, pltpu.roll(x, 7, 0))
    return op(y, pltpu.roll(y, 6, 0))


def all_sublanes(x):
    for shift in (4, 2, 1):
        x = x + pltpu.roll(x, shift, 0)
    return x


def old_mass(air_old, wide, sub):
    zero = jnp.zeros((8, LANES), jnp.float32)
    old = zero
    for c in range(wide.shape[0]):
        cols = slice(c * LANES, (c + 1) * LANES)
        for v in range(16):
            air = jnp.broadcast_to(air_old[v : v + 1, cols], (8, LANES))
            old = old + wide[c, rows(v), :] * air
    tails = []
    for t in (8, 9):
        total = zero
        for c in range(wide.shape[0]):
            cols = slice(c * LANES, (c + 1) * LANES)
            for h in (0, 8):
                at = t * 16 + h
                total = total + wide[c, at : at + 8, :] * air_old[h : h + 8, cols]
        tails.append(all_sublanes(total))
    return old, jnp.where(sub == 0, tails[0], jnp.where(sub == 4, tails[1], zero))


def gather(value, along_a, along_b, stack):
    def inner(first):
        total = low = high = None
        for q in range(4):
            x = value(first + q)
            low = x if low is None else jnp.minimum(low, x)
            high = x if high is None else jnp.maximum(high, x)
            term = along_b[q] * x
            total = term if total is None else total + term
        return total, low, high

    interp, low, high = inner(0)
    interp = interp * along_a[0]
    for i in range(1, 4):
        more, least, most = inner(4 * i)
        interp = interp + along_a[i] * more
        low, high = jnp.minimum(low, least), jnp.maximum(high, most)
    tail, tail_low, tail_high = inner(16)
    tail = group_of_four(tail * stack, jnp.add)
    tail_low = group_of_four(tail_low, jnp.minimum)
    tail_high = group_of_four(tail_high, jnp.maximum)
    return (interp, low, high), (tail, tail_low, tail_high)


def broadcast_row(ref, n, *at):
    return jnp.broadcast_to(ref[(*at, pl.ds(n, 1), slice(None))], (8, LANES))


def own_part(
    field, air_old, coord, slot, fetch,
    picks, own_out, old_out, along_a, along_b, stacked, slots,
    wide, table,
):
    chunks = slot.shape[1] // LANES
    points = slot.shape[0]
    sub = lax.broadcasted_iota(jnp.int32, (8, LANES), 0)
    for side, start in enumerate((chunks * LANES - BAND, 0)):
        picks[side] = jnp.broadcast_to(fetch[side : side + 1, :] - start, (8, LANES))
    for c in range(chunks):
        wide[c] = field[:, c * LANES : (c + 1) * LANES]
        slots[c] = slot[:, c * LANES : (c + 1) * LANES]
    for c in range(chunks):
        for v in range(REGISTERS):
            table[c, 8 * v : 8 * v + 8, :] = wide[c, rows(v), :]

    def step(k, carry):
        for u in range(OWN_UNROLL):
            n = k * OWN_UNROLL + u
            for e in range(chunks):
                where = broadcast_row(slots, n, e)
                near, chunk = where & (LANES - 1), where >> 7
                masks = [chunk == c for c in range(1, chunks)]
                for v in range(REGISTERS):
                    at = slice(8 * v, 8 * v + 8)
                    x = pick(table[0, at, :], near)
                    for c, mask in enumerate(masks):
                        x = jnp.where(mask, pick(table[c + 1, at, :], near), x)
                    own_out[n, e, at, :] = x
        return carry

    lax.fori_loop(0, points // OWN_UNROLL, step, 0)
    old_out[0], old_out[1] = old_mass(air_old, wide, sub)
    terms_a = basis(coord[0])
    terms_b = basis(coord[1])
    for c in range(chunks):
        cols = slice(c * LANES, (c + 1) * LANES)
        for i in range(4):
            along_a[i, c] = terms_a[i][:, cols]
            along_b[i, c] = terms_b[i][:, cols]
            stacked[c, pl.ds(i, points, stride=8), :] = terms_a[i][:, cols]
            stacked[c, pl.ds(i + 4, points, stride=8), :] = terms_a[i][:, cols]


def band_table(band, idx, wide, table):
    for c in range(2):
        wide[c] = band[:, c * LANES : (c + 1) * LANES]
    near, far = idx & (LANES - 1), idx >= LANES
    for v in range(REGISTERS):
        first = pick(wide[0, rows(v), :], near)
        second = pick(wide[1, rows(v), :], near)
        table[8 * v : 8 * v + 8, :] = jnp.where(far, second, first)


def right_part(right, picks, own, slots, merged_out, wide, table):
    points, chunks = own.shape[:2]
    band_table(right, picks[1], wide, table)

    def step(k, carry):
        for u in range(UNROLL):
            n = k * UNROLL + u
            for e in range(chunks):
                where = broadcast_row(slots, n, e)
                near, at_right = where & (LANES - 1), (where >> 7) == chunks + 1
                for v in range(REGISTERS):
                    at = slice(8 * v, 8 * v + 8)
                    x = pick(table[at, :], near)
                    merged_out[n, e, at, :] = jnp.where(at_right, x, own[n, e, at, :])
        return carry

    lax.fori_loop(0, points // UNROLL, step, 0)


def left_part(
    left, air_new, picks, merged, old, along_a, along_b, stacked, slots,
    clip_out, up_out, down_out, sums_out,
    wide, table, airs,
):
    points, chunks = merged.shape[:2]
    sub = lax.broadcasted_iota(jnp.int32, (8, LANES), 0)
    lane = lax.broadcasted_iota(jnp.int32, (8, LANES), 1)
    zero = jnp.zeros((8, LANES), jnp.float32)
    for c in range(chunks):
        airs[c] = air_new[:, c * LANES : (c + 1) * LANES]
    band_table(left, picks[0], wide, table)

    def group(n, e, acc):
        where = broadcast_row(slots, n, e)
        near, at_left = where & (LANES - 1), (where >> 7) == chunks

        def value(v):
            at = slice(8 * v, 8 * v + 8)
            return jnp.where(at_left, pick(table[at, :], near), merged[n, e, at, :])

        row_a, row_b = (
            [broadcast_row(ref, n, i, e) for i in range(4)] for ref in (along_a, along_b)
        )
        parts = gather(value, row_a, row_b, stacked[e, pl.ds(pl.multiple_of(8 * n, 8), 8), :])
        air = broadcast_row(airs, n, e)
        acc = list(acc)
        for h, (f, lo, hi) in enumerate(parts):
            at = (n, e, slice(8 * h, 8 * h + 8), slice(None))
            f = jnp.minimum(jnp.maximum(f, lo), hi)
            up, down = hi - f, f - lo
            clip_out[at], up_out[at], down_out[at] = f, up, down
            acc[3 * h] = acc[3 * h] - air * f
            acc[3 * h + 1] = acc[3 * h + 1] + air * up
            acc[3 * h + 2] = acc[3 * h + 2] + air * down
        return tuple(acc)

    def step(k, acc):
        for u in range(UNROLL):
            for e in range(chunks):
                acc = group(k * UNROLL + u, e, acc)
        return acc

    acc = lax.fori_loop(0, points // UNROLL, step, (old[0], zero, zero, old[1], zero, zero))
    row_of = zero
    for k in range(6):
        total = jnp.broadcast_to(jnp.sum(acc[k], axis=1, keepdims=True), (8, LANES))
        keep = lane == 8 * k + sub
        if k >= 3:
            keep = keep & ((sub & 3) == 0)
        row_of = row_of + jnp.where(keep, total, zero)
    row_of = all_sublanes(row_of)
    for k in range(sums_out.shape[0] // 8):
        sums_out[8 * k : 8 * k + 8, :] = row_of


def add_rows(parts):
    total = parts[0:8, :]
    for k in range(1, parts.shape[0] // 8):
        total = total + parts[8 * k : 8 * k + 8, :]
    return all_sublanes(total)


def relay(parts, sums_out):
    total = add_rows(parts)
    for k in range(sums_out.shape[0] // 8):
        sums_out[8 * k : 8 * k + 8, :] = total


def finish(parts, clip, up, down, new_out, wide, sent):
    sub = lax.broadcasted_iota(jnp.int32, (8, LANES), 0)
    lane = lax.broadcasted_iota(jnp.int32, (8, LANES), 1)
    total = add_rows(parts)
    sums = []
    for k in range(6):
        mine = jnp.where(lane == 8 * k + sub, total, jnp.zeros_like(total))
        sums.append(jnp.broadcast_to(jnp.sum(mine, axis=1, keepdims=True), (8, LANES)))
    ratios = []
    for h in range(2):
        short, room_up, room_down = sums[3 * h : 3 * h + 3]
        raised = short >= 0
        zero = jnp.zeros_like(short)
        ratios.append(
            (jnp.where(raised, short / room_up, zero), jnp.where(raised, zero, short / room_down))
        )
    copies = []
    for e in range(clip.shape[1]):
        for n in range(clip.shape[0]):
            for h in range(2):
                at = (n, e, slice(8 * h, 8 * h + 8), slice(None))
                new = clip[at] + ratios[h][0] * up[at] + ratios[h][1] * down[at]
                if h == 0:
                    wide[e, pl.ds(n, 8, stride=16), :] = new
                else:
                    wide[e, 128 + n : 129 + n, :] = new[0:1]
                    wide[e, 144 + n : 145 + n, :] = new[4:5]
        copy = pltpu.make_async_copy(wide.at[e], new_out.at[:, pl.ds(e * LANES, LANES)], sent.at[e])
        copy.start()
        copies.append(copy)
    for copy in copies:
        copy.wait()


def in_vmem(kernel, out_shape, count, scratch=(), work=0, out_space=pltpu.VMEM):
    spec = pl.BlockSpec(memory_space=pltpu.VMEM)
    return pl.pallas_call(
        kernel,
        out_shape=out_shape,
        in_specs=[spec] * count,
        out_specs=jax.tree.map(lambda _: pl.BlockSpec(memory_space=out_space), out_shape),
        scratch_shapes=scratch,
        cost_estimate=pl.CostEstimate(flops=work, bytes_accessed=0, transcendentals=0),
        compiler_params=pltpu.CompilerParams(vmem_limit_bytes=GRANT),
    )


def bands(field, last_out, first_out):
    last_out[...] = field[:, field.shape[1] - BAND :]
    first_out[...] = field[:, :BAND]


def on_device(tracer_old, air_old, air_new, dep_coord, dep_slot, fetch_list):
    _, tracers, points, e_dev = tracer_old.shape
    chunks = e_dev // LANES
    real, whole = tracer_old.dtype, jnp.int32
    field = tracer_old.reshape(tracers * points, e_dev)

    def shape(*dims, dtype=real):
        return jax.ShapeDtypeStruct(dims, dtype)

    band = shape(tracers * points, BAND)
    last, first = in_vmem(bands, (band, band), 1, work=LOAD)(field)
    count = lax.axis_size(SFC)
    forward = [(i, (i + 1) % count) for i in range(count)]
    backward = [(target, source) for source, target in forward]
    right = lax.ppermute(first, SFC, backward)
    left = lax.ppermute(last, SFC, forward)
    mid = shape(points, chunks, 16, LANES)
    plane, line = lax.axis_size(PLANE), lax.axis_size(LINE)
    terms = shape(4, chunks, points, LANES)
    table = pltpu.VMEM((8 * REGISTERS, LANES), real)
    wide = pltpu.VMEM((2, tracers * points, LANES), real)
    picked = shape(points, chunks, 8 * REGISTERS, LANES)
    picks, own, *rest = in_vmem(
        own_part,
        (
            shape(2, 8, LANES, dtype=whole),
            picked,
            shape(2, 8, LANES),
            terms,
            terms,
            shape(chunks, 8 * points, LANES),
            shape(chunks, points, LANES, dtype=whole),
        ),
        5,
        [
            pltpu.VMEM((chunks, tracers * points, LANES), real),
            pltpu.VMEM((chunks, 8 * REGISTERS, LANES), real),
        ],
        WORK,
    )(field, air_old[0], dep_coord[:, 0], dep_slot[0], fetch_list[0])
    merged = in_vmem(right_part, picked, 4, [wide, table], WORK)(right, picks, own, rest[-1])
    clip, up, down, sums = in_vmem(
        left_part,
        (mid, mid, mid, shape(plane, LANES)),
        4 + len(rest),
        [wide, table, pltpu.VMEM((chunks, points, LANES), real)],
    )(left, air_new[0], picks, merged, *rest)
    sums = lax.all_to_all(sums, PLANE, 0, 0, tiled=True)
    sums = in_vmem(relay, shape(line, LANES), 1)(sums)
    sums = lax.all_to_all(sums, LINE, 0, 0, tiled=True)
    new = in_vmem(
        finish,
        shape(tracers * points, e_dev),
        4,
        [
            pltpu.VMEM((chunks, tracers * points, LANES), real),
            pltpu.SemaphoreType.DMA((chunks,)),
        ],
        out_space=pl.ANY,
    )(sums, clip, up, down)
    return new.reshape(tracer_old.shape)


def solution(mesh):
    finer = Mesh(mesh.devices.reshape(32, 2, 4, 4), ("sfc_0", "sfc_1", "lev_0", "lev_1"))
    placed = (
        P(LEV, None, None, SFC),
        P(LEV, None, SFC),
        P(LEV, None, SFC),
        P(None, LEV, None, SFC),
        P(LEV, None, SFC),
        P(SFC, None, None),
    )
    return jax.shard_map(
        on_device, mesh=finer, in_specs=placed, out_specs=P(LEV, None, None, SFC), check_vma=False
    )
```

```python
import jax
import jax.numpy as jnp
from jax import lax
from jax.experimental import pallas as pl
from jax.experimental.pallas import tpu as pltpu
from jax.sharding import Mesh
from jax.sharding import PartitionSpec as P

BAND = 256
LANES = 128
SFC = ("sfc_0", "sfc_1")
LEV = ("lev_0", "lev_1")
PLANE = ("sfc_1", "lev_0", "lev_1")
LINE = "sfc_0"
NODES = (-1.0, -0.4472135954999579, 0.4472135954999579, 1.0)
REGISTERS = 20
OWN_UNROLL = 16
GRANT = 12 * 1024 * 1024
WORK = 1_000_000_000
LOAD = 10_000_000_000


def basis(coord):
    terms = []
    for first in range(4):
        term, scale = None, 1.0
        for other in range(4):
            if other != first:
                factor = coord - NODES[other]
                term = factor if term is None else term * factor
                scale *= NODES[first] - NODES[other]
        terms.append(term * (1.0 / scale))
    return terms


def rows(v):
    return pl.ds(v, 8, stride=16) if v < 16 else pl.ds(128 + v - 16, 8, stride=4)


def pick(table, idx):
    return jnp.take_along_axis(table, idx, axis=1, mode="promise_in_bounds")


def group_of_four(x, op):
    y = op(x, pltpu.roll(x, 7, 0))
    return op(y, pltpu.roll(y, 6, 0))


def all_sublanes(x):
    for shift in (4, 2, 1):
        x = x + pltpu.roll(x, shift, 0)
    return x


def old_mass(air_old, wide, sub):
    zero = jnp.zeros((8, LANES), jnp.float32)
    old = zero
    for c in range(wide.shape[0]):
        cols = slice(c * LANES, (c + 1) * LANES)
        for v in range(16):
            air = jnp.broadcast_to(air_old[v : v + 1, cols], (8, LANES))
            old = old + wide[c, rows(v), :] * air
    tails = []
    for t in (8, 9):
        total = zero
        for c in range(wide.shape[0]):
            cols = slice(c * LANES, (c + 1) * LANES)
            for h in (0, 8):
                at = t * 16 + h
                total = total + wide[c, at : at + 8, :] * air_old[h : h + 8, cols]
        tails.append(all_sublanes(total))
    return old, jnp.where(sub == 0, tails[0], jnp.where(sub == 4, tails[1], zero))


def gather(value, along_a, along_b, stack):
    def inner(first):
        total = low = high = None
        for q in range(4):
            x = value(first + q)
            low = x if low is None else jnp.minimum(low, x)
            high = x if high is None else jnp.maximum(high, x)
            term = along_b[q] * x
            total = term if total is None else total + term
        return total, low, high

    interp, low, high = inner(0)
    interp = interp * along_a[0]
    for i in range(1, 4):
        more, least, most = inner(4 * i)
        interp = interp + along_a[i] * more
        low, high = jnp.minimum(low, least), jnp.maximum(high, most)
    tail, tail_low, tail_high = inner(16)
    tail = group_of_four(tail * stack, jnp.add)
    tail_low = group_of_four(tail_low, jnp.minimum)
    tail_high = group_of_four(tail_high, jnp.maximum)
    return (interp, low, high), (tail, tail_low, tail_high)


def broadcast_row(ref, n, *at):
    return jnp.broadcast_to(ref[(*at, pl.ds(n, 1), slice(None))], (8, LANES))


def own_part(
    field, air_old, coord, slot, fetch,
    picks, own_out, old_out, along_a, along_b, stacked, slots,
    wide, table,
):
    chunks = slot.shape[1] // LANES
    points = slot.shape[0]
    sub = lax.broadcasted_iota(jnp.int32, (8, LANES), 0)
    for side, start in enumerate((chunks * LANES - BAND, 0)):
        picks[side] = jnp.broadcast_to(fetch[side : side + 1, :] - start, (8, LANES))
    for c in range(chunks):
        wide[c] = field[:, c * LANES : (c + 1) * LANES]
        slots[c] = slot[:, c * LANES : (c + 1) * LANES]
    for c in range(chunks):
        for v in range(REGISTERS):
            table[c, 8 * v : 8 * v + 8, :] = wide[c, rows(v), :]

    def step(k, carry):
        for u in range(OWN_UNROLL):
            n = k * OWN_UNROLL + u
            for e in range(chunks):
                where = broadcast_row(slots, n, e)
                near, chunk = where & (LANES - 1), where >> 7
                masks = [chunk == c for c in range(1, chunks)]
                for v in range(REGISTERS):
                    at = slice(8 * v, 8 * v + 8)
                    x = pick(table[0, at, :], near)
                    for c, mask in enumerate(masks):
                        x = jnp.where(mask, pick(table[c + 1, at, :], near), x)
                    own_out[n, e, at, :] = x
        return carry

    lax.fori_loop(0, points // OWN_UNROLL, step, 0)
    old_out[0], old_out[1] = old_mass(air_old, wide, sub)
    terms_a = basis(coord[0])
    terms_b = basis(coord[1])
    for c in range(chunks):
        cols = slice(c * LANES, (c + 1) * LANES)
        for i in range(4):
            along_a[i, c] = terms_a[i][:, cols]
            along_b[i, c] = terms_b[i][:, cols]
            stacked[c, pl.ds(i, points, stride=8), :] = terms_a[i][:, cols]
            stacked[c, pl.ds(i + 4, points, stride=8), :] = terms_a[i][:, cols]


def band_table(band, idx, wide, table):
    for c in range(2):
        wide[c] = band[:, c * LANES : (c + 1) * LANES]
    near, far = idx & (LANES - 1), idx >= LANES
    for v in range(REGISTERS):
        first = pick(wide[0, rows(v), :], near)
        second = pick(wide[1, rows(v), :], near)
        table[8 * v : 8 * v + 8, :] = jnp.where(far, second, first)


def right_part(right, picks, own, slots, merged_out, wide, table):
    points, chunks = own.shape[:2]

    @pl.when(lax.axis_index("sfc_1") == 0)
    def _():
        band_table(right, picks[1], wide, table)
        for n in range(points):
            for e in range(chunks):
                where = broadcast_row(slots, n, e)
                near, at_right = where & (LANES - 1), (where >> 7) == chunks + 1
                for v in range(REGISTERS):
                    at = slice(8 * v, 8 * v + 8)
                    x = pick(table[at, :], near)
                    merged_out[n, e, at, :] = jnp.where(at_right, x, own[n, e, at, :])


def last_part(
    left, right, air_new, picks, merged, old, along_a, along_b, stacked, slots,
    clip_out, up_out, down_out, sums_out,
    wide, table, airs,
):
    points, chunks = merged.shape[:2]
    sub = lax.broadcasted_iota(jnp.int32, (8, LANES), 0)
    lane = lax.broadcasted_iota(jnp.int32, (8, LANES), 1)
    zero = jnp.zeros((8, LANES), jnp.float32)
    for c in range(chunks):
        airs[c] = air_new[:, c * LANES : (c + 1) * LANES]

    def group(n, e, acc, sides):
        where = broadcast_row(slots, n, e)
        near, chunk = where & (LANES - 1), where >> 7
        masks = [(side, chunk == chunks + side) for side in sides]

        def value(v):
            at = slice(8 * v, 8 * v + 8)
            x = merged[n, e, at, :]
            for side, mask in masks:
                x = jnp.where(mask, pick(table[side, at, :], near), x)
            return x

        row_a, row_b = (
            [broadcast_row(ref, n, i, e) for i in range(4)] for ref in (along_a, along_b)
        )
        parts = gather(value, row_a, row_b, stacked[e, 8 * n : 8 * n + 8, :])
        air = broadcast_row(airs, n, e)
        acc = list(acc)
        for h, (f, lo, hi) in enumerate(parts):
            at = (n, e, slice(8 * h, 8 * h + 8), slice(None))
            f = jnp.minimum(jnp.maximum(f, lo), hi)
            up, down = hi - f, f - lo
            clip_out[at], up_out[at], down_out[at] = f, up, down
            acc[3 * h] = acc[3 * h] - air * f
            acc[3 * h + 1] = acc[3 * h + 1] + air * up
            acc[3 * h + 2] = acc[3 * h + 2] + air * down
        return tuple(acc)

    def run(sides):
        for side in sides:
            band_table((left, right)[side], picks[side], wide.at[side], table.at[side])
        acc = (old[0], zero, zero, old[1], zero, zero)
        for n in range(points):
            for e in range(chunks):
                acc = group(n, e, acc, sides)
        row_of = zero
        for k in range(6):
            total = jnp.broadcast_to(jnp.sum(acc[k], axis=1, keepdims=True), (8, LANES))
            keep = lane == 8 * k + sub
            if k >= 3:
                keep = keep & ((sub & 3) == 0)
            row_of = row_of + jnp.where(keep, total, zero)
        row_of = all_sublanes(row_of)
        for k in range(sums_out.shape[0] // 8):
            sums_out[8 * k : 8 * k + 8, :] = row_of

    core = lax.axis_index("sfc_1")

    @pl.when(core == 0)
    def _():
        run((0,))

    @pl.when(core != 0)
    def _():
        run((0, 1))


def add_rows(parts):
    total = parts[0:8, :]
    for k in range(1, parts.shape[0] // 8):
        total = total + parts[8 * k : 8 * k + 8, :]
    return all_sublanes(total)


def relay(parts, sums_out):
    total = add_rows(parts)
    for k in range(sums_out.shape[0] // 8):
        sums_out[8 * k : 8 * k + 8, :] = total


def finish(parts, clip, up, down, new_out, wide, sent):
    sub = lax.broadcasted_iota(jnp.int32, (8, LANES), 0)
    lane = lax.broadcasted_iota(jnp.int32, (8, LANES), 1)
    total = add_rows(parts)
    sums = []
    for k in range(6):
        mine = jnp.where(lane == 8 * k + sub, total, jnp.zeros_like(total))
        sums.append(jnp.broadcast_to(jnp.sum(mine, axis=1, keepdims=True), (8, LANES)))
    ratios = []
    for h in range(2):
        short, room_up, room_down = sums[3 * h : 3 * h + 3]
        raised = short >= 0
        zero = jnp.zeros_like(short)
        ratios.append(
            (jnp.where(raised, short / room_up, zero), jnp.where(raised, zero, short / room_down))
        )
    copies = []
    for e in range(clip.shape[1]):
        for n in range(clip.shape[0]):
            for h in range(2):
                at = (n, e, slice(8 * h, 8 * h + 8), slice(None))
                new = clip[at] + ratios[h][0] * up[at] + ratios[h][1] * down[at]
                if h == 0:
                    wide[e, pl.ds(n, 8, stride=16), :] = new
                else:
                    wide[e, 128 + n : 129 + n, :] = new[0:1]
                    wide[e, 144 + n : 145 + n, :] = new[4:5]
        copy = pltpu.make_async_copy(wide.at[e], new_out.at[:, pl.ds(e * LANES, LANES)], sent.at[e])
        copy.start()
        copies.append(copy)
    for copy in copies:
        copy.wait()


def in_vmem(kernel, out_shape, count, scratch=(), work=0, out_space=pltpu.VMEM, in_place=()):
    spec = pl.BlockSpec(memory_space=pltpu.VMEM)
    return pl.pallas_call(
        kernel,
        out_shape=out_shape,
        in_specs=[spec] * count,
        out_specs=jax.tree.map(lambda _: pl.BlockSpec(memory_space=out_space), out_shape),
        scratch_shapes=scratch,
        input_output_aliases=dict(in_place),
        cost_estimate=pl.CostEstimate(flops=work, bytes_accessed=0, transcendentals=0),
        compiler_params=pltpu.CompilerParams(vmem_limit_bytes=GRANT),
    )


def bands(field, last_out, first_out):
    last_out[...] = field[:, field.shape[1] - BAND :]
    first_out[...] = field[:, :BAND]


def on_device(tracer_old, air_old, air_new, dep_coord, dep_slot, fetch_list):
    _, tracers, points, e_dev = tracer_old.shape
    chunks = e_dev // LANES
    real, whole = tracer_old.dtype, jnp.int32
    field = tracer_old.reshape(tracers * points, e_dev)

    def shape(*dims, dtype=real):
        return jax.ShapeDtypeStruct(dims, dtype)

    band = shape(tracers * points, BAND)
    last, first = in_vmem(bands, (band, band), 1, work=LOAD)(field)
    count = lax.axis_size(SFC)
    forward = [(i, (i + 1) % count) for i in range(count)]
    backward = [(target, source) for source, target in forward]
    right = lax.ppermute(first, SFC, backward)
    left = lax.ppermute(last, SFC, forward)
    mid = shape(points, chunks, 16, LANES)
    plane, line = lax.axis_size(PLANE), lax.axis_size(LINE)
    terms = shape(4, chunks, points, LANES)
    table = pltpu.VMEM((8 * REGISTERS, LANES), real)
    wide = pltpu.VMEM((2, tracers * points, LANES), real)
    picked = shape(points, chunks, 8 * REGISTERS, LANES)
    picks, own, *rest = in_vmem(
        own_part,
        (
            shape(2, 8, LANES, dtype=whole),
            picked,
            shape(2, 8, LANES),
            terms,
            terms,
            shape(chunks, 8 * points, LANES),
            shape(chunks, points, LANES, dtype=whole),
        ),
        5,
        [
            pltpu.VMEM((chunks, tracers * points, LANES), real),
            pltpu.VMEM((chunks, 8 * REGISTERS, LANES), real),
        ],
        WORK,
    )(field, air_old[0], dep_coord[:, 0], dep_slot[0], fetch_list[0])
    merged = in_vmem(right_part, picked, 4, [wide, table], WORK, in_place=((2, 0),))(
        right, picks, own, rest[-1]
    )
    clip, up, down, sums = in_vmem(
        last_part,
        (mid, mid, mid, shape(plane, LANES)),
        5 + len(rest),
        [
            pltpu.VMEM((2, 2, tracers * points, LANES), real),
            pltpu.VMEM((2, 8 * REGISTERS, LANES), real),
            pltpu.VMEM((chunks, points, LANES), real),
        ],
    )(left, right, air_new[0], picks, merged, *rest)
    sums = lax.all_to_all(sums, PLANE, 0, 0, tiled=True)
    sums = in_vmem(relay, shape(line, LANES), 1)(sums)
    sums = lax.all_to_all(sums, LINE, 0, 0, tiled=True)
    new = in_vmem(
        finish,
        shape(tracers * points, e_dev),
        4,
        [
            pltpu.VMEM((chunks, tracers * points, LANES), real),
            pltpu.SemaphoreType.DMA((chunks,)),
        ],
        out_space=pl.ANY,
    )(sums, clip, up, down)
    return new.reshape(tracer_old.shape)


def solution(mesh):
    finer = Mesh(mesh.devices.reshape(32, 2, 4, 4), ("sfc_0", "sfc_1", "lev_0", "lev_1"))
    placed = (
        P(LEV, None, None, SFC),
        P(LEV, None, SFC),
        P(LEV, None, SFC),
        P(None, LEV, None, SFC),
        P(LEV, None, SFC),
        P(SFC, None, None),
    )
    return jax.shard_map(
        on_device, mesh=finer, in_specs=placed, out_specs=P(LEV, None, None, SFC), check_vma=False
    )
```

```python
import jax
import jax.numpy as jnp
from jax import lax
from jax.experimental import pallas as pl
from jax.experimental.pallas import tpu as pltpu
from jax.sharding import Mesh
from jax.sharding import PartitionSpec as P

BAND = 256
LANES = 128
SFC = ("sfc_0", "sfc_1")
LEV = ("lev_0", "lev_1")
PLANE = ("sfc_1", "lev_0", "lev_1")
LINE = "sfc_0"
NODES = (-1.0, -0.4472135954999579, 0.4472135954999579, 1.0)
REGISTERS = 20
OWN_UNROLL = 16
GRANT = 12 * 1024 * 1024
WORK = 1_000_000_000
LOAD = 10_000_000_000


def basis(coord):
    terms = []
    for first in range(4):
        term, scale = None, 1.0
        for other in range(4):
            if other != first:
                factor = coord - NODES[other]
                term = factor if term is None else term * factor
                scale *= NODES[first] - NODES[other]
        terms.append(term * (1.0 / scale))
    return terms


def rows(v):
    return pl.ds(v, 8, stride=16) if v < 16 else pl.ds(128 + v - 16, 8, stride=4)


def pick(table, idx):
    return jnp.take_along_axis(table, idx, axis=1, mode="promise_in_bounds")


def group_of_four(x, op):
    y = op(x, pltpu.roll(x, 7, 0))
    return op(y, pltpu.roll(y, 6, 0))


def all_sublanes(x):
    for shift in (4, 2, 1):
        x = x + pltpu.roll(x, shift, 0)
    return x


def old_mass(air_old, wide, sub):
    zero = jnp.zeros((8, LANES), jnp.float32)
    old = zero
    for c in range(wide.shape[0]):
        cols = slice(c * LANES, (c + 1) * LANES)
        for v in range(16):
            air = jnp.broadcast_to(air_old[v : v + 1, cols], (8, LANES))
            old = old + wide[c, rows(v), :] * air
    tails = []
    for t in (8, 9):
        total = zero
        for c in range(wide.shape[0]):
            cols = slice(c * LANES, (c + 1) * LANES)
            for h in (0, 8):
                at = t * 16 + h
                total = total + wide[c, at : at + 8, :] * air_old[h : h + 8, cols]
        tails.append(all_sublanes(total))
    return old, jnp.where(sub == 0, tails[0], jnp.where(sub == 4, tails[1], zero))


def gather(value, along_a, along_b, stack):
    def inner(first):
        total = low = high = None
        for q in range(4):
            x = value(first + q)
            low = x if low is None else jnp.minimum(low, x)
            high = x if high is None else jnp.maximum(high, x)
            term = along_b[q] * x
            total = term if total is None else total + term
        return total, low, high

    interp, low, high = inner(0)
    interp = interp * along_a[0]
    for i in range(1, 4):
        more, least, most = inner(4 * i)
        interp = interp + along_a[i] * more
        low, high = jnp.minimum(low, least), jnp.maximum(high, most)
    tail, tail_low, tail_high = inner(16)
    tail = group_of_four(tail * stack, jnp.add)
    tail_low = group_of_four(tail_low, jnp.minimum)
    tail_high = group_of_four(tail_high, jnp.maximum)
    return (interp, low, high), (tail, tail_low, tail_high)


def broadcast_row(ref, n, *at):
    return jnp.broadcast_to(ref[(*at, pl.ds(n, 1), slice(None))], (8, LANES))


def own_part(
    field, air_old, air_new, coord, slot, fetch,
    picks, own_out, old_out, along_a, along_b, stacked, airs, slots,
    wide, table,
):
    chunks = slot.shape[1] // LANES
    points = slot.shape[0]
    sub = lax.broadcasted_iota(jnp.int32, (8, LANES), 0)
    for side, start in enumerate((chunks * LANES - BAND, 0)):
        picks[side] = jnp.broadcast_to(fetch[side : side + 1, :] - start, (8, LANES))
    for c in range(chunks):
        wide[c] = field[:, c * LANES : (c + 1) * LANES]
        slots[c] = slot[:, c * LANES : (c + 1) * LANES]
        airs[c] = air_new[:, c * LANES : (c + 1) * LANES]
    for c in range(chunks):
        for v in range(REGISTERS):
            table[c, 8 * v : 8 * v + 8, :] = wide[c, rows(v), :]

    def step(k, carry):
        for u in range(OWN_UNROLL):
            n = k * OWN_UNROLL + u
            for e in range(chunks):
                where = broadcast_row(slots, n, e)
                near, chunk = where & (LANES - 1), where >> 7
                masks = [chunk == c for c in range(1, chunks)]
                for v in range(REGISTERS):
                    at = slice(8 * v, 8 * v + 8)
                    x = pick(table[0, at, :], near)
                    for c, mask in enumerate(masks):
                        x = jnp.where(mask, pick(table[c + 1, at, :], near), x)
                    own_out[n, e, at, :] = x
        return carry

    lax.fori_loop(0, points // OWN_UNROLL, step, 0)
    old_out[0], old_out[1] = old_mass(air_old, wide, sub)
    terms_a = basis(coord[0])
    terms_b = basis(coord[1])
    for c in range(chunks):
        cols = slice(c * LANES, (c + 1) * LANES)
        for i in range(4):
            along_a[i, c] = terms_a[i][:, cols]
            along_b[i, c] = terms_b[i][:, cols]
            stacked[c, pl.ds(i, points, stride=8), :] = terms_a[i][:, cols]
            stacked[c, pl.ds(i + 4, points, stride=8), :] = terms_a[i][:, cols]


def band_table(band, idx, wide, table):
    for c in range(2):
        wide[c] = band[:, c * LANES : (c + 1) * LANES]
    near, far = idx & (LANES - 1), idx >= LANES
    for v in range(REGISTERS):
        first = pick(wide[0, rows(v), :], near)
        second = pick(wide[1, rows(v), :], near)
        table[8 * v : 8 * v + 8, :] = jnp.where(far, second, first)


def right_part(right, picks, own, slots, merged_out, wide, table):
    points, chunks = own.shape[:2]

    @pl.when(lax.axis_index("sfc_1") == 0)
    def _():
        band_table(right, picks[1], wide, table)
        for n in range(points):
            for e in range(chunks):
                where = broadcast_row(slots, n, e)
                near, at_right = where & (LANES - 1), (where >> 7) == chunks + 1
                for v in range(REGISTERS):
                    at = slice(8 * v, 8 * v + 8)
                    x = pick(table[at, :], near)
                    merged_out[n, e, at, :] = jnp.where(at_right, x, own[n, e, at, :])


def last_part(
    left, right, picks, own, merged, old, along_a, along_b, stacked, airs, slots,
    clip_out, up_out, down_out, sums_out,
    wide, table,
):
    points, chunks = merged.shape[:2]
    sub = lax.broadcasted_iota(jnp.int32, (8, LANES), 0)
    lane = lax.broadcasted_iota(jnp.int32, (8, LANES), 1)
    zero = jnp.zeros((8, LANES), jnp.float32)

    def group(n, e, acc, sides, held):
        where = broadcast_row(slots, n, e)
        near, chunk = where & (LANES - 1), where >> 7
        masks = [(side, chunk == chunks + side) for side in sides]

        def value(v):
            at = slice(8 * v, 8 * v + 8)
            x = held[n, e, at, :]
            for side, mask in masks:
                x = jnp.where(mask, pick(table[side, at, :], near), x)
            return x

        row_a, row_b = (
            [broadcast_row(ref, n, i, e) for i in range(4)] for ref in (along_a, along_b)
        )
        parts = gather(value, row_a, row_b, stacked[e, 8 * n : 8 * n + 8, :])
        air = broadcast_row(airs, n, e)
        acc = list(acc)
        for h, (f, lo, hi) in enumerate(parts):
            at = (n, e, slice(8 * h, 8 * h + 8), slice(None))
            f = jnp.minimum(jnp.maximum(f, lo), hi)
            up, down = hi - f, f - lo
            clip_out[at], up_out[at], down_out[at] = f, up, down
            acc[3 * h] = acc[3 * h] - air * f
            acc[3 * h + 1] = acc[3 * h + 1] + air * up
            acc[3 * h + 2] = acc[3 * h + 2] + air * down
        return tuple(acc)

    def run(sides, held):
        for side in sides:
            band_table((left, right)[side], picks[side], wide.at[side], table.at[side])
        acc = (old[0], zero, zero, old[1], zero, zero)
        for n in range(points):
            for e in range(chunks):
                acc = group(n, e, acc, sides, held)
        row_of = zero
        for k in range(6):
            total = jnp.broadcast_to(jnp.sum(acc[k], axis=1, keepdims=True), (8, LANES))
            keep = lane == 8 * k + sub
            if k >= 3:
                keep = keep & ((sub & 3) == 0)
            row_of = row_of + jnp.where(keep, total, zero)
        row_of = all_sublanes(row_of)
        for k in range(sums_out.shape[0] // 8):
            sums_out[8 * k : 8 * k + 8, :] = row_of

    core = lax.axis_index("sfc_1")

    @pl.when(core == 0)
    def _():
        run((0,), merged)

    @pl.when(core != 0)
    def _():
        run((0, 1), own)


def add_rows(parts):
    total = parts[0:8, :]
    for k in range(1, parts.shape[0] // 8):
        total = total + parts[8 * k : 8 * k + 8, :]
    return all_sublanes(total)


def relay(parts, sums_out):
    total = add_rows(parts)
    for k in range(sums_out.shape[0] // 8):
        sums_out[8 * k : 8 * k + 8, :] = total


def finish(parts, clip, up, down, new_out, wide, sent):
    sub = lax.broadcasted_iota(jnp.int32, (8, LANES), 0)
    lane = lax.broadcasted_iota(jnp.int32, (8, LANES), 1)
    total = add_rows(parts)
    sums = []
    for k in range(6):
        mine = jnp.where(lane == 8 * k + sub, total, jnp.zeros_like(total))
        sums.append(jnp.broadcast_to(jnp.sum(mine, axis=1, keepdims=True), (8, LANES)))
    ratios = []
    for h in range(2):
        short, room_up, room_down = sums[3 * h : 3 * h + 3]
        raised = short >= 0
        zero = jnp.zeros_like(short)
        ratios.append(
            (jnp.where(raised, short / room_up, zero), jnp.where(raised, zero, short / room_down))
        )
    copies = []
    for e in range(clip.shape[1]):
        for n in range(clip.shape[0]):
            for h in range(2):
                at = (n, e, slice(8 * h, 8 * h + 8), slice(None))
                new = clip[at] + ratios[h][0] * up[at] + ratios[h][1] * down[at]
                if h == 0:
                    wide[e, pl.ds(n, 8, stride=16), :] = new
                else:
                    wide[e, 128 + n : 129 + n, :] = new[0:1]
                    wide[e, 144 + n : 145 + n, :] = new[4:5]
        copy = pltpu.make_async_copy(wide.at[e], new_out.at[:, pl.ds(e * LANES, LANES)], sent.at[e])
        copy.start()
        copies.append(copy)
    for copy in copies:
        copy.wait()


def in_vmem(kernel, out_shape, count, scratch=(), work=0, out_space=pltpu.VMEM):
    spec = pl.BlockSpec(memory_space=pltpu.VMEM)
    return pl.pallas_call(
        kernel,
        out_shape=out_shape,
        in_specs=[spec] * count,
        out_specs=jax.tree.map(lambda _: pl.BlockSpec(memory_space=out_space), out_shape),
        scratch_shapes=scratch,
        cost_estimate=pl.CostEstimate(flops=work, bytes_accessed=0, transcendentals=0),
        compiler_params=pltpu.CompilerParams(vmem_limit_bytes=GRANT),
    )


def bands(field, last_out, first_out):
    last_out[...] = field[:, field.shape[1] - BAND :]
    first_out[...] = field[:, :BAND]


def on_device(tracer_old, air_old, air_new, dep_coord, dep_slot, fetch_list):
    _, tracers, points, e_dev = tracer_old.shape
    chunks = e_dev // LANES
    real, whole = tracer_old.dtype, jnp.int32
    field = tracer_old.reshape(tracers * points, e_dev)

    def shape(*dims, dtype=real):
        return jax.ShapeDtypeStruct(dims, dtype)

    band = shape(tracers * points, BAND)
    last, first = in_vmem(bands, (band, band), 1, work=LOAD)(field)
    count = lax.axis_size(SFC)
    forward = [(i, (i + 1) % count) for i in range(count)]
    backward = [(target, source) for source, target in forward]
    right = lax.ppermute(first, SFC, backward)
    left = lax.ppermute(last, SFC, forward)
    mid = shape(points, chunks, 16, LANES)
    plane, line = lax.axis_size(PLANE), lax.axis_size(LINE)
    terms = shape(4, chunks, points, LANES)
    table = pltpu.VMEM((8 * REGISTERS, LANES), real)
    wide = pltpu.VMEM((2, tracers * points, LANES), real)
    picked = shape(points, chunks, 8 * REGISTERS, LANES)
    picks, own, *rest = in_vmem(
        own_part,
        (
            shape(2, 8, LANES, dtype=whole),
            picked,
            shape(2, 8, LANES),
            terms,
            terms,
            shape(chunks, 8 * points, LANES),
            shape(chunks, points, LANES),
            shape(chunks, points, LANES, dtype=whole),
        ),
        6,
        [
            pltpu.VMEM((chunks, tracers * points, LANES), real),
            pltpu.VMEM((chunks, 8 * REGISTERS, LANES), real),
        ],
        WORK,
    )(field, air_old[0], air_new[0], dep_coord[:, 0], dep_slot[0], fetch_list[0])
    merged = in_vmem(right_part, picked, 4, [wide, table], WORK)(right, picks, own, rest[-1])
    clip, up, down, sums = in_vmem(
        last_part,
        (mid, mid, mid, shape(plane, LANES)),
        5 + len(rest),
        [
            pltpu.VMEM((2, 2, tracers * points, LANES), real),
            pltpu.VMEM((2, 8 * REGISTERS, LANES), real),
        ],
    )(left, right, picks, own, merged, *rest)
    sums = lax.all_to_all(sums, PLANE, 0, 0, tiled=True)
    sums = in_vmem(relay, shape(line, LANES), 1)(sums)
    sums = lax.all_to_all(sums, LINE, 0, 0, tiled=True)
    new = in_vmem(
        finish,
        shape(tracers * points, e_dev),
        4,
        [
            pltpu.VMEM((chunks, tracers * points, LANES), real),
            pltpu.SemaphoreType.DMA((chunks,)),
        ],
        out_space=pl.ANY,
    )(sums, clip, up, down)
    return new.reshape(tracer_old.shape)


def solution(mesh):
    finer = Mesh(mesh.devices.reshape(32, 2, 4, 4), ("sfc_0", "sfc_1", "lev_0", "lev_1"))
    placed = (
        P(LEV, None, None, SFC),
        P(LEV, None, SFC),
        P(LEV, None, SFC),
        P(None, LEV, None, SFC),
        P(LEV, None, SFC),
        P(SFC, None, None),
    )
    return jax.shard_map(
        on_device, mesh=finer, in_specs=placed, out_specs=P(LEV, None, None, SFC), check_vma=False
    )
```

```python
import jax
import jax.numpy as jnp
from jax import lax
from jax.experimental import pallas as pl
from jax.experimental.pallas import tpu as pltpu
from jax.sharding import Mesh
from jax.sharding import PartitionSpec as P

BAND = 256
LANES = 128
SFC = ("sfc_0", "sfc_1")
LEV = ("lev_0", "lev_1")
PLANE = ("sfc_1", "lev_0", "lev_1")
LINE = "sfc_0"
NODES = (-1.0, -0.4472135954999579, 0.4472135954999579, 1.0)
REGISTERS = 20
OWN_UNROLL = 16
GRANT = 12 * 1024 * 1024
WORK = 1_000_000_000
LOAD = 10_000_000_000


def basis(coord):
    terms = []
    for first in range(4):
        term, scale = None, 1.0
        for other in range(4):
            if other != first:
                factor = coord - NODES[other]
                term = factor if term is None else term * factor
                scale *= NODES[first] - NODES[other]
        terms.append(term * (1.0 / scale))
    return terms


def rows(v):
    return pl.ds(v, 8, stride=16) if v < 16 else pl.ds(128 + v - 16, 8, stride=4)


def pick(table, idx):
    return jnp.take_along_axis(table, idx, axis=1, mode="promise_in_bounds")


def group_of_four(x, op):
    y = op(x, pltpu.roll(x, 7, 0))
    return op(y, pltpu.roll(y, 6, 0))


def all_sublanes(x):
    for shift in (4, 2, 1):
        x = x + pltpu.roll(x, shift, 0)
    return x


def old_mass(air_old, wide, sub):
    zero = jnp.zeros((8, LANES), jnp.float32)
    old = zero
    for c in range(wide.shape[0]):
        cols = slice(c * LANES, (c + 1) * LANES)
        for v in range(16):
            air = jnp.broadcast_to(air_old[v : v + 1, cols], (8, LANES))
            old = old + wide[c, rows(v), :] * air
    tails = []
    for t in (8, 9):
        total = zero
        for c in range(wide.shape[0]):
            cols = slice(c * LANES, (c + 1) * LANES)
            for h in (0, 8):
                at = t * 16 + h
                total = total + wide[c, at : at + 8, :] * air_old[h : h + 8, cols]
        tails.append(all_sublanes(total))
    return old, jnp.where(sub == 0, tails[0], jnp.where(sub == 4, tails[1], zero))


def gather(value, along_a, along_b, stack):
    def inner(first):
        total = low = high = None
        for q in range(4):
            x = value(first + q)
            low = x if low is None else jnp.minimum(low, x)
            high = x if high is None else jnp.maximum(high, x)
            term = along_b[q] * x
            total = term if total is None else total + term
        return total, low, high

    interp, low, high = inner(0)
    interp = interp * along_a[0]
    for i in range(1, 4):
        more, least, most = inner(4 * i)
        interp = interp + along_a[i] * more
        low, high = jnp.minimum(low, least), jnp.maximum(high, most)
    tail, tail_low, tail_high = inner(16)
    tail = group_of_four(tail * stack, jnp.add)
    tail_low = group_of_four(tail_low, jnp.minimum)
    tail_high = group_of_four(tail_high, jnp.maximum)
    return (interp, low, high), (tail, tail_low, tail_high)


def broadcast_row(ref, n, *at):
    return jnp.broadcast_to(ref[(*at, pl.ds(n, 1), slice(None))], (8, LANES))


def own_part(
    field, air_old, air_new, coord, slot, fetch,
    picks, own_out, old_out, along_a, along_b, stacked, airs, slots,
    wide, table,
):
    chunks = slot.shape[1] // LANES
    points = slot.shape[0]
    sub = lax.broadcasted_iota(jnp.int32, (8, LANES), 0)
    for side, start in enumerate((chunks * LANES - BAND, 0)):
        picks[side] = jnp.broadcast_to(fetch[side : side + 1, :] - start, (8, LANES))
    for c in range(chunks):
        wide[c] = field[:, c * LANES : (c + 1) * LANES]
        slots[c] = slot[:, c * LANES : (c + 1) * LANES]
        airs[c] = air_new[:, c * LANES : (c + 1) * LANES]
    for c in range(chunks):
        for v in range(REGISTERS):
            table[c, 8 * v : 8 * v + 8, :] = wide[c, rows(v), :]

    def step(k, carry):
        for u in range(OWN_UNROLL):
            n = k * OWN_UNROLL + u
            for e in range(chunks):
                where = broadcast_row(slots, n, e)
                near, chunk = where & (LANES - 1), where >> 7
                masks = [chunk == c for c in range(1, chunks)]
                for v in range(REGISTERS):
                    at = slice(8 * v, 8 * v + 8)
                    x = pick(table[0, at, :], near)
                    for c, mask in enumerate(masks):
                        x = jnp.where(mask, pick(table[c + 1, at, :], near), x)
                    own_out[n, e, at, :] = x
        return carry

    lax.fori_loop(0, points // OWN_UNROLL, step, 0)
    old_out[0], old_out[1] = old_mass(air_old, wide, sub)
    terms_a = basis(coord[0])
    terms_b = basis(coord[1])
    for c in range(chunks):
        cols = slice(c * LANES, (c + 1) * LANES)
        for i in range(4):
            along_a[i, c] = terms_a[i][:, cols]
            along_b[i, c] = terms_b[i][:, cols]
            stacked[c, pl.ds(i, points, stride=8), :] = terms_a[i][:, cols]
            stacked[c, pl.ds(i + 4, points, stride=8), :] = terms_a[i][:, cols]


def band_table(band, idx, table):
    near, far = idx & (LANES - 1), idx >= LANES
    for v in range(REGISTERS):
        first = pick(band[0, rows(v), :], near)
        second = pick(band[1, rows(v), :], near)
        table[8 * v : 8 * v + 8, :] = jnp.where(far, second, first)


def right_part(right, picks, own, slots, merged_out, table):
    points, chunks = own.shape[:2]

    @pl.when(lax.axis_index("sfc_1") == 0)
    def _():
        band_table(right, picks[1], table)
        for n in range(points):
            for e in range(chunks):
                where = broadcast_row(slots, n, e)
                near, at_right = where & (LANES - 1), (where >> 7) == chunks + 1
                for v in range(REGISTERS):
                    at = slice(8 * v, 8 * v + 8)
                    x = pick(table[at, :], near)
                    merged_out[n, e, at, :] = jnp.where(at_right, x, own[n, e, at, :])


def last_part(
    left, right, picks, own, merged, old, along_a, along_b, stacked, airs, slots,
    clip_out, up_out, down_out, sums_out,
    table,
):
    points, chunks = merged.shape[:2]
    sub = lax.broadcasted_iota(jnp.int32, (8, LANES), 0)
    lane = lax.broadcasted_iota(jnp.int32, (8, LANES), 1)
    zero = jnp.zeros((8, LANES), jnp.float32)

    def group(n, e, acc, sides, held):
        where = broadcast_row(slots, n, e)
        near, chunk = where & (LANES - 1), where >> 7
        masks = [(side, chunk == chunks + side) for side in sides]

        def value(v):
            at = slice(8 * v, 8 * v + 8)
            x = held[n, e, at, :]
            for side, mask in masks:
                x = jnp.where(mask, pick(table[side, at, :], near), x)
            return x

        row_a, row_b = (
            [broadcast_row(ref, n, i, e) for i in range(4)] for ref in (along_a, along_b)
        )
        parts = gather(value, row_a, row_b, stacked[e, 8 * n : 8 * n + 8, :])
        air = broadcast_row(airs, n, e)
        acc = list(acc)
        for h, (f, lo, hi) in enumerate(parts):
            at = (n, e, slice(8 * h, 8 * h + 8), slice(None))
            f = jnp.minimum(jnp.maximum(f, lo), hi)
            up, down = hi - f, f - lo
            clip_out[at], up_out[at], down_out[at] = f, up, down
            acc[3 * h] = acc[3 * h] - air * f
            acc[3 * h + 1] = acc[3 * h + 1] + air * up
            acc[3 * h + 2] = acc[3 * h + 2] + air * down
        return tuple(acc)

    def run(sides, held):
        for side in sides:
            band_table((left, right)[side], picks[side], table.at[side])
        acc = (old[0], zero, zero, old[1], zero, zero)
        for n in range(points):
            for e in range(chunks):
                acc = group(n, e, acc, sides, held)
        row_of = zero
        for k in range(6):
            total = jnp.broadcast_to(jnp.sum(acc[k], axis=1, keepdims=True), (8, LANES))
            keep = lane == 8 * k + sub
            if k >= 3:
                keep = keep & ((sub & 3) == 0)
            row_of = row_of + jnp.where(keep, total, zero)
        row_of = all_sublanes(row_of)
        for k in range(sums_out.shape[0] // 8):
            sums_out[8 * k : 8 * k + 8, :] = row_of

    core = lax.axis_index("sfc_1")

    @pl.when(core == 0)
    def _():
        run((0,), merged)

    @pl.when(core != 0)
    def _():
        run((0, 1), own)


def add_rows(parts):
    total = parts[0:8, :]
    for k in range(1, parts.shape[0] // 8):
        total = total + parts[8 * k : 8 * k + 8, :]
    return all_sublanes(total)


def relay(parts, sums_out):
    total = add_rows(parts)
    for k in range(sums_out.shape[0] // 8):
        sums_out[8 * k : 8 * k + 8, :] = total


def finish(parts, clip, up, down, new_out, wide, sent):
    sub = lax.broadcasted_iota(jnp.int32, (8, LANES), 0)
    lane = lax.broadcasted_iota(jnp.int32, (8, LANES), 1)
    total = add_rows(parts)
    sums = []
    for k in range(6):
        mine = jnp.where(lane == 8 * k + sub, total, jnp.zeros_like(total))
        sums.append(jnp.broadcast_to(jnp.sum(mine, axis=1, keepdims=True), (8, LANES)))
    ratios = []
    for h in range(2):
        short, room_up, room_down = sums[3 * h : 3 * h + 3]
        raised = short >= 0
        zero = jnp.zeros_like(short)
        ratios.append(
            (jnp.where(raised, short / room_up, zero), jnp.where(raised, zero, short / room_down))
        )
    copies = []
    for e in range(clip.shape[1]):
        for n in range(clip.shape[0]):
            for h in range(2):
                at = (n, e, slice(8 * h, 8 * h + 8), slice(None))
                new = clip[at] + ratios[h][0] * up[at] + ratios[h][1] * down[at]
                if h == 0:
                    wide[e, pl.ds(n, 8, stride=16), :] = new
                else:
                    wide[e, 128 + n : 129 + n, :] = new[0:1]
                    wide[e, 144 + n : 145 + n, :] = new[4:5]
        copy = pltpu.make_async_copy(wide.at[e], new_out.at[:, pl.ds(e * LANES, LANES)], sent.at[e])
        copy.start()
        copies.append(copy)
    for copy in copies:
        copy.wait()


def in_vmem(kernel, out_shape, count, scratch=(), work=0, out_space=pltpu.VMEM):
    spec = pl.BlockSpec(memory_space=pltpu.VMEM)
    return pl.pallas_call(
        kernel,
        out_shape=out_shape,
        in_specs=[spec] * count,
        out_specs=jax.tree.map(lambda _: pl.BlockSpec(memory_space=out_space), out_shape),
        scratch_shapes=scratch,
        cost_estimate=pl.CostEstimate(flops=work, bytes_accessed=0, transcendentals=0),
        compiler_params=pltpu.CompilerParams(vmem_limit_bytes=GRANT),
    )


def bands(field, last_out, first_out):
    for out, start in ((last_out, field.shape[1] - BAND), (first_out, 0)):
        for c in range(BAND // LANES):
            out[c] = field[:, start + c * LANES : start + (c + 1) * LANES]


def on_device(tracer_old, air_old, air_new, dep_coord, dep_slot, fetch_list):
    _, tracers, points, e_dev = tracer_old.shape
    chunks = e_dev // LANES
    real, whole = tracer_old.dtype, jnp.int32
    field = tracer_old.reshape(tracers * points, e_dev)

    def shape(*dims, dtype=real):
        return jax.ShapeDtypeStruct(dims, dtype)

    band = shape(BAND // LANES, tracers * points, LANES)
    last, first = in_vmem(bands, (band, band), 1, work=LOAD)(field)
    count = lax.axis_size(SFC)
    forward = [(i, (i + 1) % count) for i in range(count)]
    backward = [(target, source) for source, target in forward]
    right = lax.ppermute(first, SFC, backward)
    left = lax.ppermute(last, SFC, forward)
    mid = shape(points, chunks, 16, LANES)
    plane, line = lax.axis_size(PLANE), lax.axis_size(LINE)
    terms = shape(4, chunks, points, LANES)
    table = pltpu.VMEM((8 * REGISTERS, LANES), real)
    picked = shape(points, chunks, 8 * REGISTERS, LANES)
    picks, own, *rest = in_vmem(
        own_part,
        (
            shape(2, 8, LANES, dtype=whole),
            picked,
            shape(2, 8, LANES),
            terms,
            terms,
            shape(chunks, 8 * points, LANES),
            shape(chunks, points, LANES),
            shape(chunks, points, LANES, dtype=whole),
        ),
        6,
        [
            pltpu.VMEM((chunks, tracers * points, LANES), real),
            pltpu.VMEM((chunks, 8 * REGISTERS, LANES), real),
        ],
        WORK,
    )(field, air_old[0], air_new[0], dep_coord[:, 0], dep_slot[0], fetch_list[0])
    merged = in_vmem(right_part, picked, 4, [table], WORK)(right, picks, own, rest[-1])
    clip, up, down, sums = in_vmem(
        last_part,
        (mid, mid, mid, shape(plane, LANES)),
        5 + len(rest),
        [pltpu.VMEM((2, 8 * REGISTERS, LANES), real)],
    )(left, right, picks, own, merged, *rest)
    sums = lax.all_to_all(sums, PLANE, 0, 0, tiled=True)
    sums = in_vmem(relay, shape(line, LANES), 1)(sums)
    sums = lax.all_to_all(sums, LINE, 0, 0, tiled=True)
    new = in_vmem(
        finish,
        shape(tracers * points, e_dev),
        4,
        [
            pltpu.VMEM((chunks, tracers * points, LANES), real),
            pltpu.SemaphoreType.DMA((chunks,)),
        ],
        out_space=pl.ANY,
    )(sums, clip, up, down)
    return new.reshape(tracer_old.shape)


def solution(mesh):
    finer = Mesh(mesh.devices.reshape(32, 2, 4, 4), ("sfc_0", "sfc_1", "lev_0", "lev_1"))
    placed = (
        P(LEV, None, None, SFC),
        P(LEV, None, SFC),
        P(LEV, None, SFC),
        P(None, LEV, None, SFC),
        P(LEV, None, SFC),
        P(SFC, None, None),
    )
    return jax.shard_map(
        on_device, mesh=finer, in_specs=placed, out_specs=P(LEV, None, None, SFC), check_vma=False
    )
```
